16 devices in a mesh: data: 2 (over z), tp: 8 (over y, x, core).
Axes of the slice: x: 2, y: 2, z: 2, core: 2. Of those that a mesh axis runs over, the one named last changes fastest.
Arguments:
- x_in: bfloat16 [16384, 3072], P('data'), parts along dimension 0
- w_gate: bfloat16 [3072, 8192], P(None, 'tp')
- w_up: bfloat16 [3072, 8192], P(None, 'tp')
- w_down: bfloat16 [8192, 3072], P('tp')
- residual: bfloat16 [16384, 3072], P(('data', 'tp')), parts along dimension 0
- norm_gain: float32 [3072], replicated
Outputs:
- output 1: bfloat16 [16384, 3072], P(('data', 'tp')), parts along dimension 0
- output 2: bfloat16 [16384, 3072], P(('data', 'tp')), parts along dimension 0
There are 2 independent parts. The reference program is written for one: setup_inputs(seed, part) draws one part's arguments, and reference() takes and returns one part's arrays. A program takes and returns all parts, laid end to end along the dimension named above; an argument that names none is the same for every part.
All inputs are finite; a program needn't handle non-finite values.
Results may differ from the reference program's by a relative error of at most 0.00648036.
Values are sent between devices in bfloat16 or wider.
A program may use at most 1 GiB of HBM per device.

```python
import jax
import jax.numpy as jnp
from jax import lax

T = 8192
D = 3072
F = 8192
TP = 8
F_SHARD = F // TP
EPS = 1e-5


def setup_inputs(seed: int = 0, part: int = 0) -> dict:
    key = jax.random.key(seed)
    shared = jax.random.split(key, 4)
    local = jax.random.split(jax.random.fold_in(key, part), 2)
    x_in = jax.random.normal(local[0], (T, D), jnp.float32).astype(jnp.bfloat16)
    residual = jax.random.normal(local[1], (T, D), jnp.float32).astype(jnp.bfloat16)
    w_gate = (jax.random.normal(shared[0], (D, F), jnp.float32) * D ** -0.5).astype(jnp.bfloat16)
    w_up = (jax.random.normal(shared[1], (D, F), jnp.float32) * D ** -0.5).astype(jnp.bfloat16)
    w_down = (jax.random.normal(shared[2], (F, D), jnp.float32) * (2.0 / F) ** 0.5).astype(jnp.bfloat16)
    norm_gain = 1.0 + 0.3 * jax.random.normal(shared[3], (D,), jnp.float32)
    return {"x_in": x_in, "w_gate": w_gate, "w_up": w_up, "w_down": w_down, "residual": residual, "norm_gain": norm_gain}


def reference(x_in, w_gate, w_up, w_down, residual, norm_gain):
    gate_shards = w_gate.reshape(D, TP, F_SHARD).transpose(1, 0, 2)
    up_shards = w_up.reshape(D, TP, F_SHARD).transpose(1, 0, 2)
    down_shards = w_down.reshape(TP, F_SHARD, D)

    def add_shard(running, shard_w):
        gate_cols, up_cols, down_rows = shard_w
        gate_val = jnp.dot(x_in, gate_cols, preferred_element_type=jnp.float32)
        up_val = jnp.dot(x_in, up_cols, preferred_element_type=jnp.float32)
        hidden = (jax.nn.silu(gate_val) * up_val).astype(jnp.bfloat16)
        part_prod = jnp.dot(hidden, down_rows, preferred_element_type=jnp.float32).astype(jnp.bfloat16)
        return running + part_prod.astype(jnp.float32), None

    y_sum = lax.scan(add_shard, jnp.zeros((T, D), jnp.float32), (gate_shards, up_shards, down_shards))[0]
    hidden_sum = residual.astype(jnp.float32) + y_sum
    mean_sq = jnp.mean(hidden_sum * hidden_sum, axis=-1, keepdims=True)
    normed = hidden_sum * lax.rsqrt(mean_sq + EPS) * norm_gain
    return hidden_sum.astype(jnp.bfloat16), normed.astype(jnp.bfloat16)
```

```python
import jax
import jax.numpy as jnp
from jax import lax
from jax.sharding import PartitionSpec as P

EPS = 1e-5


def solution(mesh):
    tp_size = mesh.shape["tp"]

    def local_block(x_in, w_gate, w_up, w_down, residual, norm_gain):
        w_all = lax.all_gather(w_down, "tp", axis=0)
        gate_val = jnp.dot(x_in, w_gate, preferred_element_type=jnp.float32)
        up_val = jnp.dot(x_in, w_up, preferred_element_type=jnp.float32)
        hidden = (jax.nn.silu(gate_val) * up_val).astype(jnp.bfloat16)
        rows = residual.shape[0]
        received = lax.all_to_all(hidden.reshape(tp_size, rows, -1), "tp", 0, 0, tiled=True)
        h = residual.astype(jnp.float32)
        total = jnp.zeros(h.shape, jnp.float32)
        for p in range(tp_size):
            part = jnp.dot(received[p], w_all[p], preferred_element_type=jnp.float32)
            total = total + lax.reduce_precision(part, 8, 7)
        h = h + total
        mean_sq = jnp.mean(h * h, axis=-1, keepdims=True)
        normed = h * lax.rsqrt(mean_sq + EPS) * norm_gain
        return h.astype(jnp.bfloat16), normed.astype(jnp.bfloat16)

    row_spec = P(("data", "tp"), None)
    return jax.shard_map(local_block, mesh=mesh, in_specs=(P("data", None), P(None, "tp"), P(None, "tp"), P("tp", None), row_spec, P(None)), out_specs=(row_spec, row_spec), check_vma=False)
```

```python
import functools

import jax
import jax.numpy as jnp
from jax import lax
from jax.experimental import pallas as pl
from jax.experimental.pallas import tpu as pltpu
from jax.sharding import PartitionSpec as P

EPS = 1e-5
MESH = pl.DeviceIdType.MESH
F32 = jnp.float32
BF16 = jnp.bfloat16


def block_kernel(x_ref, wg_ref, wu_ref, wd_ref, res_ref, gain_ref, h_ref, n_ref, wall_ref, gout, gin, w_send, w_recv, g_send, g_recv):
    p = lax.axis_index("tp")
    z = lax.axis_index("data")
    core, px, py = p % 2, (p // 2) % 2, p // 4
    rows = wd_ref.shape[0]
    half, quarter = rows // 2, rows // 4
    cols = wg_ref.shape[1]
    width = wd_ref.shape[1]
    blocks = 16

    def peer(r):
        return p + (r % 2) * (1 - 2 * core) + ((r // 2) % 2) * (2 - 4 * px) + (r // 4) * (4 - 8 * py)

    def tp(r):
        return {"tp": peer(r)}

    twin = {"data": 1 - z}

    barrier = pltpu.get_barrier_semaphore()
    for r in range(1, 8):
        pl.semaphore_signal(barrier, inc=1, device_id=tp(r), device_id_type=MESH)
    pl.semaphore_signal(barrier, inc=1, device_id=twin, device_id_type=MESH)
    pl.semaphore_wait(barrier, 8)

    mine, other = z * half, (1 - z) * half
    q0, q1 = pl.ds(mine, quarter), pl.ds(mine + quarter, quarter)
    hm, ho = pl.ds(mine, half), pl.ds(other, half)
    whole = pl.ds(0, rows)
    events = [
        (0, 2, q0, tp(2)),
        (0, 2, q1, tp(2)),
        (0, 4, q1, tp(4)),
        (0, 4, q0, tp(4)),
        (0, 1, whole, tp(1)),
        (2, 6, q0, tp(4)),
        (2, 2, q0, twin),
        (4, 6, q1, tp(2)),
        (4, 4, q1, twin),
        (2, 2, q1, twin),
        (2, 3, hm, tp(1)),
        (4, 4, q0, twin),
        (4, 5, hm, tp(1)),
        (6, 6, q0, twin),
        (6, 6, q1, twin),
        (6, 7, hm, tp(1)),
        (2, 3, ho, tp(1)),
        (4, 5, ho, tp(1)),
        (6, 7, ho, tp(1)),
    ]

    def w_copy(e):
        src, dst, where, target = events[e]
        src_ref = wd_ref.at[where] if src == 0 else wall_ref.at[src, where]
        return pltpu.make_async_remote_copy(src_ref=src_ref, dst_ref=wall_ref.at[dst, where], send_sem=w_send.at[e], recv_sem=w_recv.at[e], device_id=target, device_id_type=MESH)

    def w_start(*ids):
        for e in ids:
            w_copy(e).start()

    def w_wait(*ids):
        for e in ids:
            w_copy(e).wait_recv()

    def place(j):
        m = j % 6
        t = m % 3
        r = jnp.where(j < 12, 6 - 4 * t + 6 * (t // 2) + m // 3, 1 - (j - 12) // 2)
        return r, jnp.where(j < 12, j // 6, j % 2)

    def g_copy(j, r, h):
        return pltpu.make_async_remote_copy(src_ref=gout.at[j], dst_ref=gin.at[r - 1, pl.ds(h * half, half)], send_sem=g_send.at[j], recv_sem=g_recv.at[r * 2 + h], device_id=tp(r), device_id_type=MESH)

    w_start(0, 2, 1, 3, 4)

    def produce(xbuf, wg, wu, x_sem, wg_sem, wu_sem):
        def x_copy(j):
            r, h = place(j)
            start = pl.multiple_of(peer(r) * rows + h * half, half)
            return pltpu.make_async_copy(x_ref.at[pl.ds(start, half)], xbuf.at[j % 2], x_sem.at[j % 2])

        wg_copy = pltpu.make_async_copy(wg_ref, wg, wg_sem)
        wu_copy = pltpu.make_async_copy(wu_ref, wu, wu_sem)
        x_copy(0).start()
        wg_copy.start()
        wu_copy.start()
        wg_copy.wait()
        wu_copy.wait()

        def step(j, carry):
            x_copy(j).wait()

            @pl.when(j + 1 < blocks)
            def _():
                x_copy(j + 1).start()

            @pl.loop(0, cols // 256)
            def _(n):
                tile = pl.ds(pl.multiple_of(n * 256, 256), 256)
                xb = xbuf[j % 2]
                gate = jnp.dot(xb, wg[:, tile], preferred_element_type=F32)
                up = jnp.dot(xb, wu[:, tile], preferred_element_type=F32)
                gout[j, :, tile] = (jax.nn.silu(gate) * up).astype(BF16)

            r, h = place(j)

            @pl.when(j < 14)
            def _():
                g_copy(j, r, h).start()

            @pl.when(j == 5)
            def _():
                w_wait(0, 2)
                w_start(5, 7, 6, 8)

            @pl.when(j == 10)
            def _():
                w_wait(1, 3)
                w_start(9, 11, 10, 12)

            return carry

        lax.fori_loop(0, blocks, step, 0)

    pl.run_scoped(
        produce,
        pltpu.VMEM((2, half, wg_ref.shape[0]), BF16),
        pltpu.VMEM(wg_ref.shape, BF16),
        pltpu.VMEM(wu_ref.shape, BF16),
        pltpu.SemaphoreType.DMA((2,)),
        pltpu.SemaphoreType.DMA,
        pltpu.SemaphoreType.DMA,
    )

    def consume(acc, wbuf, wb_sem, res_sem, out_sem):
        tile_n = 512

        def load(r, slot):
            src = wd_ref if r == 0 else wall_ref.at[r]
            return pltpu.make_async_copy(src, wbuf.at[slot], wb_sem.at[slot])

        def add(r, h, slot, first=False):
            if r:
                g_copy(0, r, h).wait_recv()
            top = h * half

            @pl.loop(0, width // tile_n)
            def _(n):
                tile = pl.ds(pl.multiple_of(n * tile_n, tile_n), tile_n)
                act = gout[14 + h] if r == 0 else gin[r - 1, pl.ds(top, half)]
                part = jnp.dot(act, wbuf[slot, :, tile], preferred_element_type=F32).astype(BF16).astype(F32)
                if first:
                    acc[pl.ds(top, half), tile] = part
                else:
                    acc[pl.ds(top, half), tile] += part

        def finish(h):
            top = h * half
            chunk, sub = 128, 32
            res = pltpu.make_async_copy(res_ref.at[pl.ds(top, half)], wbuf.at[1, pl.ds(0, half)], res_sem)
            res.start()
            res.wait()
            copies = []
            for k in range(half // chunk):
                @pl.loop(0, chunk // sub)
                def _(i):
                    at = pl.multiple_of(k * chunk + i * sub, sub)
                    h32 = wbuf[1, pl.ds(at, sub)].astype(F32) + acc[pl.ds(top + at, sub)]
                    mean_sq = jnp.sum(h32 * h32, axis=-1, keepdims=True) * (1.0 / width)
                    wbuf[0, pl.ds(at, sub)] = h32.astype(BF16)
                    wbuf[0, pl.ds(half + at, sub)] = (h32 * lax.rsqrt(mean_sq + EPS) * gain_ref[...]).astype(BF16)

                place_out = pl.ds(top + k * chunk, chunk)
                copies.append(pltpu.make_async_copy(wbuf.at[0, pl.ds(k * chunk, chunk)], h_ref.at[place_out], out_sem.at[2 * k]))
                copies.append(pltpu.make_async_copy(wbuf.at[0, pl.ds(half + k * chunk, chunk)], n_ref.at[place_out], out_sem.at[2 * k + 1]))
                copies[-2].start()
                copies[-1].start()
            for copy in copies:
                copy.wait()

        def run(steps, first=False):
            load(steps[0][0], 0).start()
            for i, (r, halves) in enumerate(steps):
                load(r, i % 2).wait()
                if i + 1 < len(steps):
                    load(steps[i + 1][0], (i + 1) % 2).start()
                for h in halves:
                    add(r, h, i % 2, first and i == 0)

        w_wait(4)
        run([(0, (0, 1)), (1, (0, 1))], first=True)
        w_wait(5, 7)
        w_start(13, 14, 15)
        w_wait(6, 9)
        w_start(16)
        w_wait(8, 11)
        w_start(17)
        w_wait(10, 16, 12, 17)
        run([(2, (0,)), (4, (0,)), (3, (0,)), (5, (0,))])
        w_wait(13, 14)
        w_start(18)
        w_wait(15, 18)
        run([(6, (0,)), (7, (0,))])
        finish(0)
        run([(6, (1,)), (2, (1,)), (4, (1,)), (7, (1,)), (3, (1,)), (5, (1,))])
        finish(1)

    pl.run_scoped(
        consume,
        pltpu.VMEM((rows, width), F32),
        pltpu.VMEM((2, rows, width), BF16),
        pltpu.SemaphoreType.DMA((2,)),
        pltpu.SemaphoreType.DMA,
        pltpu.SemaphoreType.DMA((8,)),
    )

    for e in range(len(events)):
        w_copy(e).wait_send()

    def drain(j, carry):
        r, h = place(j)
        g_copy(j, r, h).wait_send()
        return carry

    lax.fori_loop(0, 14, drain, 0)


def solution(mesh):
    def local_block(x_in, w_gate, w_up, w_down, residual, norm_gain):
        rows, width = residual.shape
        cols = w_gate.shape[1]
        any_spec = pl.BlockSpec(memory_space=pl.ANY)
        h_out, normed, _ = pl.pallas_call(
            block_kernel,
            out_shape=(
                jax.ShapeDtypeStruct((rows, width), BF16),
                jax.ShapeDtypeStruct((rows, width), BF16),
                jax.ShapeDtypeStruct((8, rows, width), BF16),
            ),
            in_specs=[any_spec] * 5 + [pl.BlockSpec(memory_space=pltpu.VMEM)],
            out_specs=(any_spec, any_spec, any_spec),
            scratch_shapes=[
                pltpu.VMEM((16, rows // 2, cols), BF16),
                pltpu.VMEM((7, rows, cols), BF16),
                pltpu.SemaphoreType.DMA((19,)),
                pltpu.SemaphoreType.DMA((19,)),
                pltpu.SemaphoreType.DMA((16,)),
                pltpu.SemaphoreType.DMA((16,)),
            ],
            compiler_params=pltpu.CompilerParams(collective_id=0, has_side_effects=True, vmem_limit_bytes=66_000_000),
        )(x_in, w_gate, w_up, w_down, residual, norm_gain.reshape(1, width))
        return h_out, normed

    row_spec = P(("data", "tp"), None)
    return jax.shard_map(local_block, mesh=mesh, in_specs=(P("data", None), P(None, "tp"), P(None, "tp"), P("tp", None), row_spec, P(None)), out_specs=(row_spec, row_spec), check_vma=False)
```

```python
import functools

import jax
import jax.numpy as jnp
from jax import lax
from jax.experimental import pallas as pl
from jax.experimental.pallas import tpu as pltpu
from jax.sharding import PartitionSpec as P

EPS = 1e-5
MESH = pl.DeviceIdType.MESH
F32 = jnp.float32
BF16 = jnp.bfloat16


def block_kernel(x_ref, wg_ref, wu_ref, wd_ref, res_ref, gain_ref, h_ref, n_ref, wall_ref, gout, gin, w_send, w_recv, g_send, g_recv):
    p = lax.axis_index("tp")
    z = lax.axis_index("data")
    core, px, py = p % 2, (p // 2) % 2, p // 4
    rows = wd_ref.shape[0]
    half, quarter = rows // 2, rows // 4
    cols = wg_ref.shape[1]
    width = wd_ref.shape[1]
    blocks = 16
    gate_step = 4

    def peer(r):
        return p + (r % 2) * (1 - 2 * core) + ((r // 2) % 2) * (2 - 4 * px) + (r // 4) * (4 - 8 * py)

    def tp(r):
        return {"tp": peer(r)}

    twin = {"data": 1 - z}

    mine, other = z * half, (1 - z) * half
    q0, q1 = pl.ds(mine, quarter), pl.ds(mine + quarter, quarter)
    hm, ho = pl.ds(mine, half), pl.ds(other, half)
    whole = pl.ds(0, rows)
    events = [
        (0, 2, q0, tp(2)),
        (0, 2, q1, tp(2)),
        (0, 4, q1, tp(4)),
        (0, 4, q0, tp(4)),
        (0, 1, whole, tp(1)),
        (2, 6, q0, tp(4)),
        (2, 2, q0, twin),
        (4, 6, q1, tp(2)),
        (4, 4, q1, twin),
        (2, 2, q1, twin),
        (2, 3, hm, tp(1)),
        (4, 4, q0, twin),
        (4, 5, hm, tp(1)),
        (6, 6, q0, twin),
        (6, 6, q1, twin),
        (6, 7, hm, tp(1)),
        (2, 3, ho, tp(1)),
        (4, 5, ho, tp(1)),
        (6, 7, ho, tp(1)),
    ]

    def w_copy(e):
        src, dst, where, target = events[e]
        src_ref = wd_ref.at[where] if src == 0 else wall_ref.at[src, where]
        return pltpu.make_async_remote_copy(src_ref=src_ref, dst_ref=wall_ref.at[dst, where], send_sem=w_send.at[e], recv_sem=w_recv.at[e], device_id=target, device_id_type=MESH)

    def w_start(*ids):
        for e in ids:
            w_copy(e).start()

    def w_wait(*ids):
        for e in ids:
            w_copy(e).wait_recv()

    def place(j):
        near_r, near_h = 2 + 2 * (j % 2) + (j % 4) // 2, j // 4
        far_r, far_h = 6 + j % 2, (j - 8) // 2
        r = jnp.where(j < 8, near_r, jnp.where(j < 12, far_r, 1 - (j - 12) // 2))
        return r, jnp.where(j < 8, near_h, jnp.where(j < 12, far_h, j % 2))

    def g_copy(j, r, h, s):
        src = gout.at[j, pl.ds(s * quarter, quarter)]
        dst = gin.at[r - 1, pl.ds(h * half + s * quarter, quarter)]
        return pltpu.make_async_remote_copy(src_ref=src, dst_ref=dst, send_sem=g_send.at[2 * j + s], recv_sem=g_recv.at[4 * r + 2 * h + s], device_id=tp(r), device_id_type=MESH)

    def g_start(j):
        r, h = place(j)
        for s in range(2):
            g_copy(j, r, h, s).start()

    def produce(xbuf, wg, wu, x_sem, wg_sem, wu_sem):
        def x_copy(j):
            r, h = place(j)
            start = pl.multiple_of(peer(r) * rows + h * half, half)
            return pltpu.make_async_copy(x_ref.at[pl.ds(start, half)], xbuf.at[j % 2], x_sem.at[j % 2])

        wg_copy = pltpu.make_async_copy(wg_ref, wg, wg_sem)
        wu_copy = pltpu.make_async_copy(wu_ref, wu, wu_sem)
        x_copy(0).start()
        wg_copy.start()
        wu_copy.start()

        barrier = pltpu.get_barrier_semaphore()
        for r in range(1, 8):
            pl.semaphore_signal(barrier, inc=1, device_id=tp(r), device_id_type=MESH)
        pl.semaphore_signal(barrier, inc=1, device_id=twin, device_id_type=MESH)
        pl.semaphore_wait(barrier, 8)

        w_start(0, 2, 1, 3, 4)
        wg_copy.wait()
        wu_copy.wait()

        def send(j, carry):
            g_start(j)
            return carry

        def step(j, carry):
            x_copy(j).wait()

            @pl.when(j + 1 < blocks)
            def _():
                x_copy(j + 1).start()

            @pl.loop(0, cols // 256)
            def _(n):
                tile = pl.ds(pl.multiple_of(n * 256, 256), 256)
                xb = xbuf[j % 2]
                gate = jnp.dot(xb, wg[:, tile], preferred_element_type=F32)
                up = jnp.dot(xb, wu[:, tile], preferred_element_type=F32)
                gout[j, :, tile] = (jax.nn.silu(gate) * up).astype(BF16)

            @pl.when(j == gate_step)
            def _():
                w_wait(0, 2)
                w_start(5, 7, 6, 8)
                lax.fori_loop(0, gate_step, send, 0)

            @pl.when((j >= gate_step) & (j < 14))
            def _():
                g_start(j)

            @pl.when(j == 9)
            def _():
                w_wait(1, 3)
                w_start(9, 11, 10, 12)

            return carry

        lax.fori_loop(0, blocks, step, 0)

    pl.run_scoped(
        produce,
        pltpu.VMEM((2, half, wg_ref.shape[0]), BF16),
        pltpu.VMEM(wg_ref.shape, BF16),
        pltpu.VMEM(wu_ref.shape, BF16),
        pltpu.SemaphoreType.DMA((2,)),
        pltpu.SemaphoreType.DMA,
        pltpu.SemaphoreType.DMA,
    )

    def consume(acc, wbuf, rbuf, wb_sem, res_sem, out_sem):
        tile_n = 512

        def load(r, slot):
            src = wd_ref if r == 0 else wall_ref.at[r]
            return pltpu.make_async_copy(src, wbuf.at[slot], wb_sem.at[slot])

        def add(r, h, slot, first=False, part=None):
            subs = (0, 1) if part is None else (part,)
            if r:
                for s in subs:
                    g_copy(0, r, h, s).wait_recv()
            count = quarter * len(subs)
            inner = pl.ds(subs[0] * quarter, count)
            outer = pl.ds(h * half + subs[0] * quarter, count)

            @pl.loop(0, width // tile_n)
            def _(n):
                tile = pl.ds(pl.multiple_of(n * tile_n, tile_n), tile_n)
                act = gout[14 + h, inner] if r == 0 else gin[r - 1, outer]
                prod = jnp.dot(act, wbuf[slot, :, tile], preferred_element_type=F32).astype(BF16).astype(F32)
                if first:
                    acc[outer, tile] = prod
                else:
                    acc[outer, tile] += prod

        def res_copy(h):
            return pltpu.make_async_copy(res_ref.at[pl.ds(h * half, half)], rbuf, res_sem)

        def out_copies(h, k):
            there = pl.ds(h * half + k * chunk, chunk)
            return (
                pltpu.make_async_copy(wbuf.at[0, pl.ds(k * chunk, chunk)], h_ref.at[there], out_sem.at[2 * k]),
                pltpu.make_async_copy(wbuf.at[0, pl.ds(half + k * chunk, chunk)], n_ref.at[there], out_sem.at[2 * k + 1]),
            )

        chunk, sub = 128, 32

        def finish(h, ks):
            for k in ks:
                @pl.loop(0, chunk // sub)
                def _(i):
                    at = pl.multiple_of(k * chunk + i * sub, sub)
                    h32 = rbuf[pl.ds(at, sub)].astype(F32) + acc[pl.ds(h * half + at, sub)]
                    mean_sq = jnp.sum(h32 * h32, axis=-1, keepdims=True) * (1.0 / width)
                    wbuf[0, pl.ds(at, sub)] = h32.astype(BF16)
                    wbuf[0, pl.ds(half + at, sub)] = (h32 * lax.rsqrt(mean_sq + EPS) * gain_ref[...]).astype(BF16)

                for copy in out_copies(h, k):
                    copy.start()

        def finish_wait(h):
            for k in range(half // chunk):
                for copy in out_copies(h, k):
                    copy.wait()

        def run(steps, first=False):
            load(steps[0][0], 0).start()
            for i, (r, halves) in enumerate(steps):
                load(r, i % 2).wait()
                if i + 1 < len(steps):
                    load(steps[i + 1][0], (i + 1) % 2).start()
                for h in halves:
                    add(r, h, i % 2, first and i == 0)

        res_copy(0).start()
        w_wait(5, 7)
        w_start(13, 14, 15)
        w_wait(4)
        run([(0, (0, 1)), (1, (0, 1))], first=True)
        w_wait(6, 9)
        w_start(16)
        w_wait(8, 11)
        w_start(17)
        run([(2, (0,)), (4, (0,))])
        w_wait(10, 16, 12, 17)
        run([(3, (0,)), (5, (0,)), (2, (1,)), (4, (1,)), (3, (1,)), (5, (1,))])
        w_wait(13, 14)
        w_start(18)
        load(6, 0).start()
        load(6, 0).wait()
        add(6, 0, 0)
        w_wait(15, 18)
        load(7, 1).start()
        load(7, 1).wait()
        add(7, 0, 1)
        add(6, 1, 0)
        res_copy(0).wait()
        finish(0, range(4))
        res_copy(1).start()
        add(7, 1, 1, part=0)
        finish_wait(0)
        res_copy(1).wait()
        finish(1, (0, 1))
        add(7, 1, 1, part=1)
        finish(1, (2, 3))
        finish_wait(1)

    pl.run_scoped(
        consume,
        pltpu.VMEM((rows, width), F32),
        pltpu.VMEM((2, rows, width), BF16),
        pltpu.VMEM((half, width), BF16),
        pltpu.SemaphoreType.DMA((2,)),
        pltpu.SemaphoreType.DMA,
        pltpu.SemaphoreType.DMA((8,)),
    )

    for e in range(len(events)):
        w_copy(e).wait_send()

    def drain(j, carry):
        r, h = place(j)
        for s in range(2):
            g_copy(j, r, h, s).wait_send()
        return carry

    lax.fori_loop(0, 14, drain, 0)


def solution(mesh):
    def local_block(x_in, w_gate, w_up, w_down, residual, norm_gain):
        rows, width = residual.shape
        cols = w_gate.shape[1]
        any_spec = pl.BlockSpec(memory_space=pl.ANY)
        h_out, normed, _ = pl.pallas_call(
            block_kernel,
            out_shape=(
                jax.ShapeDtypeStruct((rows, width), BF16),
                jax.ShapeDtypeStruct((rows, width), BF16),
                jax.ShapeDtypeStruct((8, rows, width), BF16),
            ),
            in_specs=[any_spec] * 5 + [pl.BlockSpec(memory_space=pltpu.VMEM)],
            out_specs=(any_spec, any_spec, any_spec),
            scratch_shapes=[
                pltpu.VMEM((16, rows // 2, cols), BF16),
                pltpu.VMEM((7, rows, cols), BF16),
                pltpu.SemaphoreType.DMA((19,)),
                pltpu.SemaphoreType.DMA((19,)),
                pltpu.SemaphoreType.DMA((32,)),
                pltpu.SemaphoreType.DMA((32,)),
            ],
            compiler_params=pltpu.CompilerParams(collective_id=0, has_side_effects=True, vmem_limit_bytes=66_000_000),
        )(x_in, w_gate, w_up, w_down, residual, norm_gain.reshape(1, width))
        return h_out, normed

    row_spec = P(("data", "tp"), None)
    return jax.shard_map(local_block, mesh=mesh, in_specs=(P("data", None), P(None, "tp"), P(None, "tp"), P("tp", None), row_spec, P(None)), out_specs=(row_spec, row_spec), check_vma=False)
```

```python
import functools

import jax
import jax.numpy as jnp
from jax import lax
from jax.experimental import pallas as pl
from jax.experimental.pallas import tpu as pltpu
from jax.sharding import PartitionSpec as P

EPS = 1e-5
MESH = pl.DeviceIdType.MESH
F32 = jnp.float32
BF16 = jnp.bfloat16


def block_kernel(x_ref, wg_ref, wu_ref, wd_ref, res_ref, gain_ref, h_ref, n_ref, wall_ref, gout, gin, w_send, w_recv, g_send, g_recv):
    p = lax.axis_index("tp")
    z = lax.axis_index("data")
    core, px, py = p % 2, (p // 2) % 2, p // 4
    rows = wd_ref.shape[0]
    half, quarter, piece = rows // 2, rows // 4, rows // 8
    cols = wg_ref.shape[1]
    width = wd_ref.shape[1]
    blocks = 16
    gate_step = 4

    def peer(r):
        return p + (r % 2) * (1 - 2 * core) + ((r // 2) % 2) * (2 - 4 * px) + (r // 4) * (4 - 8 * py)

    def tp(r):
        return {"tp": peer(r)}

    twin = {"data": 1 - z}

    mine, other = z * half, (1 - z) * half
    q0, q1 = pl.ds(mine, quarter), pl.ds(mine + quarter, quarter)
    hm, ho = pl.ds(mine, half), pl.ds(other, half)
    whole = pl.ds(0, rows)
    events = [
        (0, 2, q0, tp(2)),
        (0, 2, q1, tp(2)),
        (0, 4, q1, tp(4)),
        (0, 4, q0, tp(4)),
        (0, 1, whole, tp(1)),
        (2, 6, q0, tp(4)),
        (2, 2, q0, twin),
        (4, 6, q1, tp(2)),
        (4, 4, q1, twin),
        (2, 2, q1, twin),
        (2, 3, hm, tp(1)),
        (4, 4, q0, twin),
        (4, 5, hm, tp(1)),
        (6, 6, q0, twin),
        (6, 6, q1, twin),
        (6, 7, hm, tp(1)),
        (2, 3, ho, tp(1)),
        (4, 5, ho, tp(1)),
        (6, 7, ho, tp(1)),
    ]

    def w_copy(e):
        src, dst, where, target = events[e]
        src_ref = wd_ref.at[where] if src == 0 else wall_ref.at[src, where]
        return pltpu.make_async_remote_copy(src_ref=src_ref, dst_ref=wall_ref.at[dst, where], send_sem=w_send.at[e], recv_sem=w_recv.at[e], device_id=target, device_id_type=MESH)

    def w_start(*ids):
        for e in ids:
            w_copy(e).start()

    def w_wait(*ids):
        for e in ids:
            w_copy(e).wait_recv()

    def place(j):
        near_r, near_h = 2 + 2 * (j % 2) + (j % 4) // 2, j // 4
        far_r, far_h = 6 + j % 2, (j - 8) // 2
        r = jnp.where(j < 8, near_r, jnp.where(j < 12, far_r, 1 - (j - 12) // 2))
        return r, jnp.where(j < 8, near_h, jnp.where(j < 12, far_h, j % 2))

    def g_copy(j, r, h, s):
        src = gout.at[j, pl.ds(s * piece, piece)]
        dst = gin.at[r - 1, pl.ds(h * half + s * piece, piece)]
        return pltpu.make_async_remote_copy(src_ref=src, dst_ref=dst, send_sem=g_send.at[4 * j + s], recv_sem=g_recv.at[8 * r + 4 * h + s], device_id=tp(r), device_id_type=MESH)

    def g_start(j):
        r, h = place(j)
        for s in range(4):
            g_copy(j, r, h, s).start()

    def produce(xbuf, wg, wu, x_sem, wg_sem, wu_sem):
        def x_copy(j):
            r, h = place(j)
            start = pl.multiple_of(peer(r) * rows + h * half, half)
            return pltpu.make_async_copy(x_ref.at[pl.ds(start, half)], xbuf.at[j % 2], x_sem.at[j % 2])

        wg_copy = pltpu.make_async_copy(wg_ref, wg, wg_sem)
        wu_copy = pltpu.make_async_copy(wu_ref, wu, wu_sem)
        x_copy(0).start()
        wg_copy.start()
        wu_copy.start()

        barrier = pltpu.get_barrier_semaphore()
        for r in range(1, 8):
            pl.semaphore_signal(barrier, inc=1, device_id=tp(r), device_id_type=MESH)
        pl.semaphore_signal(barrier, inc=1, device_id=twin, device_id_type=MESH)
        pl.semaphore_wait(barrier, 8)

        w_start(0, 2, 1, 3, 4)
        wg_copy.wait()
        wu_copy.wait()

        def send(j, carry):
            g_start(j)
            return carry

        def step(j, carry):
            x_copy(j).wait()

            @pl.when(j + 1 < blocks)
            def _():
                x_copy(j + 1).start()

            @pl.loop(0, cols // 256)
            def _(n):
                tile = pl.ds(pl.multiple_of(n * 256, 256), 256)
                xb = xbuf[j % 2]
                gate = jnp.dot(xb, wg[:, tile], preferred_element_type=F32)
                up = jnp.dot(xb, wu[:, tile], preferred_element_type=F32)
                gout[j, :, tile] = (jax.nn.silu(gate) * up).astype(BF16)

            @pl.when(j == gate_step)
            def _():
                w_wait(0, 2)
                w_start(5, 7, 6, 8)
                lax.fori_loop(0, gate_step, send, 0)

            @pl.when((j >= gate_step) & (j < 14))
            def _():
                g_start(j)

            @pl.when(j == 9)
            def _():
                w_wait(1, 3)
                w_start(9, 11, 10, 12)

            return carry

        lax.fori_loop(0, blocks, step, 0)

    pl.run_scoped(
        produce,
        pltpu.VMEM((2, half, wg_ref.shape[0]), BF16),
        pltpu.VMEM(wg_ref.shape, BF16),
        pltpu.VMEM(wu_ref.shape, BF16),
        pltpu.SemaphoreType.DMA((2,)),
        pltpu.SemaphoreType.DMA,
        pltpu.SemaphoreType.DMA,
    )

    def consume(acc, wbuf, rbuf, wb_sem, res_sem):
        tile_n = 512

        def load(r, slot):
            src = wd_ref if r == 0 else wall_ref.at[r]
            return pltpu.make_async_copy(src, (h_ref, wbuf)[slot], wb_sem.at[slot])

        def add(r, h, slot, first=False, subs=(0, 1, 2, 3)):
            if r:
                for s in subs:
                    g_copy(0, r, h, s).wait_recv()
            count = piece * len(subs)
            inner = pl.ds(subs[0] * piece, count)
            outer = pl.ds(h * half + subs[0] * piece, count)

            @pl.loop(0, width // tile_n)
            def _(n):
                tile = pl.ds(pl.multiple_of(n * tile_n, tile_n), tile_n)
                act = gout[14 + h, inner] if r == 0 else gin[r - 1, outer]
                prod = jnp.dot(act, (h_ref, wbuf)[slot][:, tile], preferred_element_type=F32).astype(BF16).astype(F32)
                if first:
                    acc[outer, tile] = prod
                else:
                    acc[outer, tile] += prod

        def res_copy(h, k):
            return pltpu.make_async_copy(res_ref.at[pl.ds(h * half + k * chunk, chunk)], rbuf.at[k % 2], res_sem.at[k % 2])

        chunk, sub = 128, 32

        def finish(h, ks):
            for k in ks:
                res_copy(h, k).wait()
                @pl.loop(0, chunk // sub)
                def _(i):
                    at = pl.multiple_of(i * sub, sub)
                    there = pl.ds(h * half + k * chunk + at, sub)
                    h32 = rbuf[k % 2, pl.ds(at, sub)].astype(F32) + acc[there]
                    mean_sq = jnp.sum(h32 * h32, axis=-1, keepdims=True) * (1.0 / width)
                    h_ref[there] = h32.astype(BF16)
                    n_ref[there] = (h32 * lax.rsqrt(mean_sq + EPS) * gain_ref[...]).astype(BF16)

                if 4 * h + k + 2 < 8:
                    res_copy(h + (k + 2) // 4, (k + 2) % 4).start()

        def run(steps, first=False):
            load(steps[0][0], 0).start()
            for i, (r, halves) in enumerate(steps):
                load(r, i % 2).wait()
                if i + 1 < len(steps):
                    load(steps[i + 1][0], (i + 1) % 2).start()
                for h in halves:
                    add(r, h, i % 2, first and i == 0)

        res_copy(0, 0).start()
        res_copy(0, 1).start()
        w_wait(5, 7)
        w_start(13, 14, 15)
        w_wait(4)
        run([(0, (0, 1)), (1, (0, 1))], first=True)
        w_wait(6, 9)
        w_start(16)
        w_wait(8, 11)
        w_start(17)
        run([(2, (0,)), (4, (0,))])
        w_wait(10, 16, 12, 17)
        run([(3, (0,)), (5, (0,)), (2, (1,)), (4, (1,)), (3, (1,)), (5, (1,))])
        w_wait(13, 14)
        w_start(18)
        load(6, 0).start()
        load(6, 0).wait()
        add(6, 0, 0)
        w_wait(15, 18)
        load(7, 1).start()
        load(7, 1).wait()
        add(7, 0, 1)
        add(6, 1, 0)
        finish(0, range(4))
        add(7, 1, 1, subs=(0, 1))
        finish(1, (0, 1))
        add(7, 1, 1, subs=(2,))
        finish(1, (2,))
        add(7, 1, 1, subs=(3,))
        finish(1, (3,))

    pl.run_scoped(
        consume,
        pltpu.VMEM((rows, width), F32),
        pltpu.VMEM((rows, width), BF16),
        pltpu.VMEM((2, 128, width), BF16),
        pltpu.SemaphoreType.DMA((2,)),
        pltpu.SemaphoreType.DMA((2,)),
    )

    for e in range(len(events)):
        w_copy(e).wait_send()

    def drain(j, carry):
        r, h = place(j)
        for s in range(4):
            g_copy(j, r, h, s).wait_send()
        return carry

    lax.fori_loop(0, 14, drain, 0)


def solution(mesh):
    def local_block(x_in, w_gate, w_up, w_down, residual, norm_gain):
        rows, width = residual.shape
        cols = w_gate.shape[1]
        any_spec = pl.BlockSpec(memory_space=pl.ANY)
        vm = pl.BlockSpec(memory_space=pltpu.VMEM)
        h_out, normed, _ = pl.pallas_call(
            block_kernel,
            out_shape=(
                pltpu.VMEM((rows, width), BF16),
                pltpu.VMEM((rows, width), BF16),
                jax.ShapeDtypeStruct((8, rows, width), BF16),
            ),
            in_specs=[any_spec] * 5 + [pl.BlockSpec(memory_space=pltpu.VMEM)],
            out_specs=(vm, vm, any_spec),
            scratch_shapes=[
                pltpu.VMEM((16, rows // 2, cols), BF16),
                pltpu.VMEM((7, rows, cols), BF16),
                pltpu.SemaphoreType.DMA((19,)),
                pltpu.SemaphoreType.DMA((19,)),
                pltpu.SemaphoreType.DMA((64,)),
                pltpu.SemaphoreType.DMA((64,)),
            ],
            compiler_params=pltpu.CompilerParams(collective_id=0, has_side_effects=True, vmem_limit_bytes=53_700_000),
        )(x_in, w_gate, w_up, w_down, residual, norm_gain.reshape(1, width))
        return h_out, normed

    row_spec = P(("data", "tp"), None)
    return jax.shard_map(local_block, mesh=mesh, in_specs=(P("data", None), P(None, "tp"), P(None, "tp"), P("tp", None), row_spec, P(None)), out_specs=(row_spec, row_spec), check_vma=False)
```

```python
import functools

import jax
import jax.numpy as jnp
from jax import lax
from jax.experimental import pallas as pl
from jax.experimental.pallas import tpu as pltpu
from jax.sharding import PartitionSpec as P

EPS = 1e-5
MESH = pl.DeviceIdType.MESH
F32 = jnp.float32
BF16 = jnp.bfloat16


def block_kernel(x_ref, wg_ref, wu_ref, wd_ref, res_ref, gain_ref, h_ref, n_ref, wbuf, part_ref, act_ref, rbuf, wall_ref, gout, gin, w_send, w_recv, g_send, g_recv):
    p = lax.axis_index("tp")
    z = lax.axis_index("data")
    core, px, py = p % 2, (p // 2) % 2, p // 4
    rows = wd_ref.shape[0]
    half, quarter, piece = rows // 2, rows // 4, rows // 8
    cols = wg_ref.shape[1]
    width = wd_ref.shape[1]
    blocks = 16
    gate_step = 4

    def peer(r):
        return p + (r % 2) * (1 - 2 * core) + ((r // 2) % 2) * (2 - 4 * px) + (r // 4) * (4 - 8 * py)

    def tp(r):
        return {"tp": peer(r)}

    twin = {"data": 1 - z}

    mine, other = z * half, (1 - z) * half
    q0, q1 = pl.ds(mine, quarter), pl.ds(mine + quarter, quarter)
    hm, ho = pl.ds(mine, half), pl.ds(other, half)
    whole = pl.ds(0, rows)
    events = [
        (0, 2, q0, tp(2)),
        (0, 2, q1, tp(2)),
        (0, 4, q1, tp(4)),
        (0, 4, q0, tp(4)),
        (0, 1, whole, tp(1)),
        (2, 6, q0, tp(4)),
        (2, 2, q0, twin),
        (4, 6, q1, tp(2)),
        (4, 4, q1, twin),
        (2, 2, q1, twin),
        (2, 3, hm, tp(1)),
        (4, 4, q0, twin),
        (4, 5, hm, tp(1)),
        (6, 6, q0, twin),
        (6, 6, q1, twin),
        (6, 7, hm, tp(1)),
        (2, 3, ho, tp(1)),
        (4, 5, ho, tp(1)),
        (6, 7, ho, tp(1)),
    ]

    def w_copy(e):
        src, dst, where, target = events[e]
        src_ref = wd_ref.at[where] if src == 0 else wall_ref.at[src, where]
        return pltpu.make_async_remote_copy(src_ref=src_ref, dst_ref=wall_ref.at[dst, where], send_sem=w_send.at[e], recv_sem=w_recv.at[e], device_id=target, device_id_type=MESH)

    def w_start(*ids):
        for e in ids:
            w_copy(e).start()

    def w_wait(*ids):
        for e in ids:
            w_copy(e).wait_recv()

    def place(j):
        near_r, near_h = 2 + 2 * (j % 2) + (j % 4) // 2, j // 4
        far_r, far_h = 6 + j % 2, (j - 8) // 2
        r = jnp.where(j < 8, near_r, jnp.where(j < 12, far_r, 1 - (j - 12) // 2))
        return r, jnp.where(j < 8, near_h, jnp.where(j < 12, far_h, j % 2))

    def g_copy(j, r, h, s):
        src = gout.at[j, pl.ds(s * piece, piece)]
        dst = gin.at[r - 1, pl.ds(h * half + s * piece, piece)]
        return pltpu.make_async_remote_copy(src_ref=src, dst_ref=dst, send_sem=g_send.at[4 * j + s], recv_sem=g_recv.at[8 * r + 4 * h + s], device_id=tp(r), device_id_type=MESH)

    def g_start(j):
        r, h = place(j)
        for s in range(4):
            g_copy(j, r, h, s).start()

    def g_wait_send(j):
        r, h = place(j)
        for s in range(4):
            g_copy(j, r, h, s).wait_send()

    def produce(wg, wu, x_sem, wg_sem, wu_sem):
        def x_copy(j):
            r, h = place(j)
            start = pl.multiple_of(peer(r) * rows + h * half, half)
            return pltpu.make_async_copy(x_ref.at[pl.ds(start, half)], n_ref.at[pl.ds((j % 2) * half, half)], x_sem.at[j % 2])

        wg_copy = pltpu.make_async_copy(wg_ref, wg, wg_sem)
        wu_copy = pltpu.make_async_copy(wu_ref, wu, wu_sem)
        x_copy(0).start()
        wg_copy.start()
        wu_copy.start()

        barrier = pltpu.get_barrier_semaphore()
        for r in range(1, 8):
            pl.semaphore_signal(barrier, inc=1, device_id=tp(r), device_id_type=MESH)
        pl.semaphore_signal(barrier, inc=1, device_id=twin, device_id_type=MESH)
        pl.semaphore_wait(barrier, 8)

        w_start(0, 2, 1, 3, 4)
        wg_copy.wait()
        wu_copy.wait()

        def send(j, carry):
            g_start(j)
            return carry

        def step(j, carry):
            x_copy(j).wait()
            slot = jnp.where(j < 14, j, j - 2)

            @pl.when(j + 1 < blocks)
            def _():
                x_copy(j + 1).start()

            @pl.when(j >= 14)
            def _():
                g_wait_send(j - 2)

            @pl.loop(0, cols // 256)
            def _(n):
                tile = pl.ds(pl.multiple_of(n * 256, 256), 256)
                xb = n_ref[pl.ds(pl.multiple_of((j % 2) * half, half), half)]
                gate = jnp.dot(xb, wg[:, tile], preferred_element_type=F32)
                up = jnp.dot(xb, wu[:, tile], preferred_element_type=F32)
                gout[slot, :, tile] = (jax.nn.silu(gate) * up).astype(BF16)

            @pl.when(j == gate_step)
            def _():
                w_wait(0, 2)
                w_start(5, 7, 6, 8)
                lax.fori_loop(0, gate_step, send, 0)

            @pl.when((j >= gate_step) & (j < 14))
            def _():
                g_start(j)

            @pl.when(j == 9)
            def _():
                w_wait(1, 3)
                w_start(9, 11, 10, 12)

            return carry

        lax.fori_loop(0, blocks, step, 0)

    pl.run_scoped(
        produce,
        pltpu.VMEM(wg_ref.shape, BF16),
        pltpu.VMEM(wu_ref.shape, BF16),
        pltpu.SemaphoreType.DMA((2,)),
        pltpu.SemaphoreType.DMA,
        pltpu.SemaphoreType.DMA,
    )

    def consume(acc, wb_sem, res_sem):
        tile_n = 512

        def load(r, slot):
            src = wd_ref if r == 0 else wall_ref.at[r]
            return pltpu.make_async_copy(src, (h_ref, wbuf)[slot], wb_sem.at[slot])

        def add(r, h, slot, first=False, subs=(0, 1, 2, 3)):
            if r:
                for s in subs:
                    g_copy(0, r, h, s).wait_recv()
            count = piece * len(subs)
            inner = pl.ds(subs[0] * piece, count)
            outer = pl.ds(h * half + subs[0] * piece, count)

            @pl.loop(0, width // tile_n)
            def _(n):
                tile = pl.ds(pl.multiple_of(n * tile_n, tile_n), tile_n)
                act = gout[12 + h, inner] if r == 0 else gin[r - 1, outer]
                prod = jnp.dot(act, (h_ref, wbuf)[slot][:, tile], preferred_element_type=F32).astype(BF16).astype(F32)
                if first:
                    acc[outer, tile] = prod
                else:
                    acc[outer, tile] += prod

        def res_copy(h, k):
            return pltpu.make_async_copy(res_ref.at[pl.ds(h * half + k * chunk, chunk)], rbuf.at[k % 2], res_sem.at[k % 2])

        chunk, sub = 64, 32

        def finish(h, ks):
            for k in ks:
                res_copy(h, k).wait()
                @pl.loop(0, chunk // sub)
                def _(i):
                    at = pl.multiple_of(i * sub, sub)
                    there = pl.ds(h * half + k * chunk + at, sub)
                    h32 = rbuf[k % 2, pl.ds(at, sub)].astype(F32) + acc[there]
                    mean_sq = jnp.sum(h32 * h32, axis=-1, keepdims=True) * (1.0 / width)
                    h_ref[there] = h32.astype(BF16)
                    n_ref[there] = (h32 * lax.rsqrt(mean_sq + EPS) * gain_ref[...]).astype(BF16)

                if 8 * h + k + 2 < 16:
                    res_copy(h + (k + 2) // 8, (k + 2) % 8).start()

        def run(steps, first=False):
            load(steps[0][0], 0).start()
            for i, (r, halves) in enumerate(steps):
                load(r, i % 2).wait()
                if i + 1 < len(steps):
                    load(steps[i + 1][0], (i + 1) % 2).start()
                for h in halves:
                    add(r, h, i % 2, first and i == 0)

        res_copy(0, 0).start()
        res_copy(0, 1).start()
        w_wait(5, 7)
        w_start(13, 14, 15)
        w_wait(4)
        run([(0, (0, 1)), (1, (0, 1))], first=True)
        w_wait(6, 9)
        w_start(16)
        w_wait(8, 11)
        w_start(17)
        run([(2, (0,)), (4, (0,))])
        w_wait(10, 16, 12, 17)
        run([(3, (0,)), (5, (0,)), (2, (1,)), (4, (1,)), (3, (1,)), (5, (1,))])
        w_wait(13, 14)
        w_start(18)
        load(6, 0).start()
        load(6, 0).wait()
        add(6, 0, 0)
        w_wait(15, 18)
        load(7, 1).start()
        load(7, 1).wait()
        add(7, 0, 1)
        add(6, 1, 0)
        finish(0, range(8))
        add(7, 1, 1, subs=(0, 1))
        finish(1, range(4))
        add(7, 1, 1, subs=(2,))
        finish(1, (4, 5))
        tail = pl.ds(rows - piece, piece)
        part_ref[...] = acc[tail]
        res_copy(1, 6).wait()
        res_copy(1, 7).wait()
        g_copy(0, 7, 1, 3).wait_recv()
        act_ref[...] = gin[6, tail]

    pl.run_scoped(
        consume,
        pltpu.VMEM((rows, width), F32),
        pltpu.SemaphoreType.DMA((2,)),
        pltpu.SemaphoreType.DMA((2,)),
    )

    for e in range(len(events)):
        w_copy(e).wait_send()

    def drain(j, carry):
        g_wait_send(j)
        return carry

    lax.fori_loop(0, 12, drain, 0)


def tail_kernel(h_ref, n_ref, w_ref, part_ref, act_ref, res_ref, gain_ref, h_out, n_out, total, tail_h, tail_n, sem):
    rows, width = h_ref.shape
    piece = part_ref.shape[0]
    done, tail = pl.ds(0, rows - piece), pl.ds(rows - piece, piece)
    copies = [
        pltpu.make_async_copy(h_ref.at[done], h_out.at[done], sem.at[0]),
        pltpu.make_async_copy(n_ref.at[done], n_out.at[done], sem.at[1]),
        pltpu.make_async_copy(tail_h, h_out.at[tail], sem.at[2]),
        pltpu.make_async_copy(tail_n, n_out.at[tail], sem.at[3]),
    ]
    copies[0].start()
    copies[1].start()
    tile_n, sub = 512, 32

    @pl.loop(0, width // tile_n)
    def _(n):
        tile = pl.ds(pl.multiple_of(n * tile_n, tile_n), tile_n)
        prod = jnp.dot(act_ref[...], w_ref[:, tile], preferred_element_type=F32)
        total[:, tile] = part_ref[:, tile] + prod.astype(BF16).astype(F32)

    @pl.loop(0, piece // sub)
    def _(i):
        at = pl.ds(pl.multiple_of(i * sub, sub), sub)
        within = pl.ds(pl.multiple_of((i % 2) * sub, sub), sub)
        h32 = res_ref[i // 2, within].astype(F32) + total[at]
        mean_sq = jnp.sum(h32 * h32, axis=-1, keepdims=True) * (1.0 / width)
        tail_h[at] = h32.astype(BF16)
        tail_n[at] = (h32 * lax.rsqrt(mean_sq + EPS) * gain_ref[...]).astype(BF16)

    copies[2].start()
    copies[3].start()
    for copy in copies:
        copy.wait()


def solution(mesh):
    def local_block(x_in, w_gate, w_up, w_down, residual, norm_gain):
        rows, width = residual.shape
        cols = w_gate.shape[1]
        any_spec = pl.BlockSpec(memory_space=pl.ANY)
        vm = pl.BlockSpec(memory_space=pltpu.VMEM)
        piece = rows // 8
        gain = norm_gain.reshape(1, width)
        *held, _ = pl.pallas_call(
            block_kernel,
            out_shape=(
                pltpu.VMEM((rows, width), BF16),
                pltpu.VMEM((rows, width), BF16),
                pltpu.VMEM((rows, width), BF16),
                pltpu.VMEM((piece, width), F32),
                pltpu.VMEM((piece, cols), BF16),
                pltpu.VMEM((2, piece // 2, width), BF16),
                jax.ShapeDtypeStruct((8, rows, width), BF16),
            ),
            in_specs=[any_spec] * 5 + [vm],
            out_specs=(vm,) * 6 + (any_spec,),
            scratch_shapes=[
                pltpu.VMEM((14, rows // 2, cols), BF16),
                pltpu.VMEM((7, rows, cols), BF16),
                pltpu.SemaphoreType.DMA((19,)),
                pltpu.SemaphoreType.DMA((19,)),
                pltpu.SemaphoreType.DMA((64,)),
                pltpu.SemaphoreType.DMA((64,)),
            ],
            compiler_params=pltpu.CompilerParams(collective_id=0, has_side_effects=True, vmem_limit_bytes=45_100_000),
        )(x_in, w_gate, w_up, w_down, residual, gain)
        return pl.pallas_call(
            tail_kernel,
            out_shape=(jax.ShapeDtypeStruct((rows, width), BF16), jax.ShapeDtypeStruct((rows, width), BF16)),
            in_specs=[vm] * 7,
            out_specs=(any_spec, any_spec),
            scratch_shapes=[
                pltpu.VMEM((piece, width), F32),
                pltpu.VMEM((piece, width), BF16),
                pltpu.VMEM((piece, width), BF16),
                pltpu.SemaphoreType.DMA((4,)),
            ],
            compiler_params=pltpu.CompilerParams(vmem_limit_bytes=8_000_000),
        )(*held, gain)

    row_spec = P(("data", "tp"), None)
    return jax.shard_map(local_block, mesh=mesh, in_specs=(P("data", None), P(None, "tp"), P(None, "tp"), P("tp", None), row_spec, P(None)), out_specs=(row_spec, row_spec), check_vma=False)
```

```python
import functools

import jax
import jax.numpy as jnp
from jax import lax
from jax.experimental import pallas as pl
from jax.experimental.pallas import tpu as pltpu
from jax.sharding import PartitionSpec as P

EPS = 1e-5
MESH = pl.DeviceIdType.MESH
F32 = jnp.float32
BF16 = jnp.bfloat16


def block_kernel(x_ref, wg_ref, wu_ref, wd_ref, res_ref, gain_ref, h_ref, n_ref, wbuf, part_ref, act_ref, wall_ref, gout, gin, w_send, w_recv, g_send, g_recv, q_send, q_recv, s_send, s_recv):
    p = lax.axis_index("tp")
    z = lax.axis_index("data")
    core, px, py = p % 2, (p // 2) % 2, p // 4
    rows = wd_ref.shape[0]
    half, quarter, piece = rows // 2, rows // 4, rows // 8
    cols = wg_ref.shape[1]
    width = wd_ref.shape[1]
    blocks = 16
    own_cols = cols * 3 // 4
    share = cols - own_cols
    depth = wg_ref.shape[0]
    deep = depth // 6

    def peer(r):
        return p + (r % 2) * (1 - 2 * core) + ((r // 2) % 2) * (2 - 4 * px) + (r // 4) * (4 - 8 * py)

    def tp(r):
        return {"tp": peer(r)}

    twin = {"data": 1 - z}

    mine, other = z * half, (1 - z) * half
    first = 13 * rows // 64
    q0, q1 = pl.ds(mine, first), pl.ds(mine + first, half - first)
    hm, ho = pl.ds(mine, half), pl.ds(other, half)
    whole = pl.ds(0, rows)
    events = [
        (0, 2, q0, tp(2)),
        (0, 2, q1, tp(2)),
        (0, 4, q1, tp(4)),
        (0, 4, q0, tp(4)),
        (0, 1, whole, tp(1)),
        (2, 6, q0, tp(4)),
        (2, 2, q0, twin),
        (4, 6, q1, tp(2)),
        (4, 4, q1, twin),
        (2, 2, q1, twin),
        (2, 3, hm, tp(1)),
        (4, 4, q0, twin),
        (4, 5, hm, tp(1)),
        (6, 6, q0, twin),
        (6, 6, q1, twin),
        (6, 7, hm, tp(1)),
        (2, 3, ho, tp(1)),
        (4, 5, ho, tp(1)),
        (6, 7, ho, tp(1)),
    ]

    def w_copy(e):
        src, dst, where, target = events[e]
        src_ref = wd_ref.at[where] if src == 0 else wall_ref.at[src, where]
        return pltpu.make_async_remote_copy(src_ref=src_ref, dst_ref=wall_ref.at[dst, where], send_sem=w_send.at[e], recv_sem=w_recv.at[e], device_id=target, device_id_type=MESH)

    def w_start(*ids):
        for e in ids:
            w_copy(e).start()

    def w_wait(*ids):
        for e in ids:
            w_copy(e).wait_recv()

    def place(j):
        g = j // 4
        return jnp.where(j < 12, 2 + 4 * g - 6 * (g // 2) + (j // 2) % 2, 1 - (j - 12) // 2), j % 2

    def g_copy(j, r, h, count):
        src = gout.at[j, :, pl.ds(0, count)]
        dst = gin.at[r - 1, pl.ds(h * half, half), pl.ds(0, count)]
        return pltpu.make_async_remote_copy(src_ref=src, dst_ref=dst, send_sem=g_send.at[j], recv_sem=g_recv.at[2 * r + h], device_id=tp(r), device_id_type=MESH)

    def g_start(j, count):
        r, h = place(j)
        g_copy(j, r, h, count).start()

    def g_wait_send(j, count):
        r, h = place(j)
        g_copy(j, r, h, count).wait_send()

    def last_copy(s):
        where = pl.ds(s * piece, piece)
        src = gout.at[7, where, pl.ds(0, own_cols)]
        dst = gin.at[6, pl.ds(half + s * piece, piece), pl.ds(0, own_cols)]
        return pltpu.make_async_remote_copy(src_ref=src, dst_ref=dst, send_sem=g_send.at[14 + s], recv_sem=g_recv.at[16 + s], device_id=tp(7), device_id_type=MESH)

    def stage(j):
        return jnp.where(j < 12, j - 4, j - 10)

    def s_copy(j, r, h):
        shared = pl.ds(own_cols, share)
        return pltpu.make_async_remote_copy(src_ref=gout.at[stage(j), :, shared], dst_ref=gin.at[r + 1, pl.ds(h * half, half), shared], send_sem=s_send.at[j - 8], recv_sem=s_recv.at[2 * r + h], device_id=tp(r), device_id_type=MESH)

    def s_start(j):
        r, h = place(j)
        s_copy(j, r, h).start()

    def q_where(k):
        at = (k % 2) * (depth // 2) + (3 * z + k // 2) * share
        return wbuf.at[pl.ds(0, deep), pl.ds(pl.multiple_of(at, share), share)]

    def q_copy(k, src, sem, target):
        return pltpu.make_async_remote_copy(src_ref=src, dst_ref=q_where(k), send_sem=q_send.at[sem], recv_sem=q_recv.at[sem], device_id=target, device_id_type=MESH)

    def q_first(k):
        src = (wg_ref, wu_ref)[k % 2]
        at = pl.multiple_of((3 * z + k // 2) * deep, deep)
        return q_copy(k, src.at[pl.ds(at, deep), pl.ds(own_cols, share)], k, tp(2))

    def q_arrived(k):
        return q_copy(k, q_where(k), k, tp(2))

    def q_swap(k):
        return q_copy(k, q_where(k), 6 + k, twin)

    def produce(wg, wu, x_sem, wg_sem, wu_sem):
        def x_copy(j):
            r, h = place(j)
            start = pl.multiple_of(peer(r) * rows + h * half, half)
            return pltpu.make_async_copy(x_ref.at[pl.ds(start, half)], n_ref.at[pl.ds((j % 2) * half, half)], x_sem.at[j % 2])

        wg_copy = pltpu.make_async_copy(wg_ref, wg, wg_sem)
        wu_copy = pltpu.make_async_copy(wu_ref, wu, wu_sem)
        x_copy(0).start()
        wg_copy.start()
        wu_copy.start()

        barrier = pltpu.get_barrier_semaphore()
        for r in range(1, 8):
            pl.semaphore_signal(barrier, inc=1, device_id=tp(r), device_id_type=MESH)
        pl.semaphore_signal(barrier, inc=1, device_id=twin, device_id_type=MESH)
        pl.semaphore_wait(barrier, 8)

        for k in range(6):
            q_first(k).start()
        w_start(0, 2, 1, 3, 4)
        wg_copy.wait()
        wu_copy.wait()

        def send_near(j, carry):
            g_start(j, own_cols)
            return carry

        def send_wide(j, carry):
            g_start(j, cols)
            s_start(j)
            return carry

        def step(j, carry):
            x_copy(j).wait()
            slot = jnp.where(j < 14, j, j - 2)
            r, h = place(j)
            xrows = pl.ds(pl.multiple_of((j % 2) * half, half), half)

            @pl.when(j + 1 < blocks)
            def _():
                x_copy(j + 1).start()

            @pl.when(j >= 14)
            def _():
                g_wait_send(j - 2, cols)

            @pl.loop(0, 3)
            def _(n):
                tile = pl.ds(pl.multiple_of(n * 256, 256), 256)
                xb = n_ref[xrows]
                gate = jnp.dot(xb, wg[:, tile], preferred_element_type=F32)
                up = jnp.dot(xb, wu[:, tile], preferred_element_type=F32)
                gout[slot, :, tile] = (jax.nn.silu(gate) * up).astype(BF16)

            @pl.when(j >= 8)
            def _():
                tile = pl.ds(own_cols, share)
                xb = n_ref[xrows]
                gate = jnp.dot(xb, wg[:, tile], preferred_element_type=F32)
                up = jnp.dot(xb, wu[:, tile], preferred_element_type=F32)
                gout[slot, :, tile] = (jax.nn.silu(gate) * up).astype(BF16)

            @pl.when(j < 6)
            def _():
                q_arrived(j).wait_recv()
                q_swap(j).start()

            @pl.when(j == 6)
            def _():
                w_wait(2)
                w_start(7, 8)

            @pl.when(j == 7)
            def _():
                lax.fori_loop(0, 7, send_near, 0)
                for s in range(4):
                    last_copy(s).start()

            @pl.when(j == 8)
            def _():
                for k in range(6):
                    q_swap(k).wait()

            @pl.when(j == 9)
            def _():
                w_wait(0)
                w_start(5, 6)

            @pl.when(j >= 8)
            def _():
                @pl.loop(0, 4)
                def _(t):
                    top = t * piece
                    xt = pl.ds(pl.multiple_of((j % 2) * half + top, piece), piece)

                    def product(base):
                        total = None
                        for k in range(6):
                            part = jnp.dot(n_ref[xt, k * deep:(k + 1) * deep], wbuf[0:deep, base + k * share:base + (k + 1) * share], preferred_element_type=F32)
                            total = part if total is None else total + part
                        return total

                    val = (jax.nn.silu(product(0)) * product(depth // 2)).astype(BF16)

                    @pl.when(j < 14)
                    def _():
                        gout[stage(j), pl.ds(pl.multiple_of(top, piece), piece), own_cols:] = val

                    @pl.when(j >= 14)
                    def _():
                        gin[1, pl.ds(pl.multiple_of(h * half + top, piece), piece), own_cols:] = val

            @pl.when(j == 9)
            def _():
                lax.fori_loop(8, 10, send_wide, 0)

            @pl.when((j >= 10) & (j < 14))
            def _():
                g_start(j, cols)
                s_start(j)

            @pl.when(j == 10)
            def _():
                w_wait(3)
                w_start(11, 12)

            @pl.when(j == 13)
            def _():
                w_wait(1)
                w_start(9, 10)

            return carry

        lax.fori_loop(0, blocks, step, 0)

    pl.run_scoped(
        produce,
        pltpu.VMEM(wg_ref.shape, BF16),
        pltpu.VMEM(wu_ref.shape, BF16),
        pltpu.SemaphoreType.DMA((2,)),
        pltpu.SemaphoreType.DMA,
        pltpu.SemaphoreType.DMA,
    )

    def drain_near(j, carry):
        g_wait_send(j, own_cols)
        return carry

    def drain_wide(j, carry):
        g_wait_send(j, cols)
        return carry

    def drain_shared(j, carry):
        r, h = place(j)
        s_copy(j, r, h).wait_send()
        return carry

    def consume(acc, wb_sem, res_sem):
        tile_n = 512

        def load(r, slot):
            src = wd_ref if r == 0 else wall_ref.at[r]
            return pltpu.make_async_copy(src, (h_ref, wbuf)[slot], wb_sem.at[slot])

        def add(r, h, slot, first=False, subs=(0, 1, 2, 3)):
            if r:
                if (r, h) == (7, 1):
                    for s in subs:
                        last_copy(s).wait_recv()
                else:
                    g_copy(0, r, h, own_cols if r in (2, 3, 6, 7) else cols).wait_recv()
            if r in (3, 6, 7) and subs[0] == 0:
                s_copy(8, r - 2, h).wait_recv()
            count = piece * len(subs)
            inner = pl.ds(subs[0] * piece, count)
            outer = pl.ds(h * half + subs[0] * piece, count)

            @pl.loop(0, width // tile_n)
            def _(n):
                tile = pl.ds(pl.multiple_of(n * tile_n, tile_n), tile_n)
                act = gout[12 + h, inner] if r == 0 else gin[r - 1, outer]
                prod = jnp.dot(act, (h_ref, wbuf)[slot][:, tile], preferred_element_type=F32).astype(BF16).astype(F32)
                if first:
                    acc[outer, tile] = prod
                else:
                    acc[outer, tile] += prod

        def add_residual():
            copy = pltpu.make_async_copy(res_ref, h_ref, res_sem)
            copy.start()
            copy.wait()

            @pl.loop(0, rows // 32)
            def _(i):
                at = pl.ds(pl.multiple_of(i * 32, 32), 32)
                acc[at] += h_ref[at].astype(F32)

        sub = 32

        def finish(h, s0, count):
            @pl.loop(0, count * piece // sub)
            def _(i):
                there = pl.ds(pl.multiple_of(h * half + s0 * piece + i * sub, sub), sub)
                h32 = acc[there]
                mean_sq = jnp.sum(h32 * h32, axis=-1, keepdims=True) * (1.0 / width)
                h_ref[there] = h32.astype(BF16)
                n_ref[there] = (h32 * lax.rsqrt(mean_sq + EPS) * gain_ref[...]).astype(BF16)

        def run(steps, first=False):
            load(steps[0][0], 0).start()
            for i, (r, halves) in enumerate(steps):
                load(r, i % 2).wait()
                if i + 1 < len(steps):
                    load(steps[i + 1][0], (i + 1) % 2).start()
                for h in halves:
                    add(r, h, i % 2, first and i == 0)

        w_wait(5)
        w_start(13)
        w_wait(4)
        run([(0, (0, 1)), (1, (0, 1))], first=True)
        w_wait(7)
        w_start(14, 15)
        w_wait(8, 11)
        w_start(17)
        run([(4, (0, 1))])
        w_wait(12, 17)
        run([(5, (0, 1))])
        w_wait(6, 9)
        w_start(16)
        run([(2, (0, 1))])
        w_wait(10, 16)
        run([(3, (0, 1))])
        for e in range(13):
            w_copy(e).wait_send()
        for k in range(6):
            q_arrived(k).wait_send()
        lax.fori_loop(0, 4, drain_near, 0)
        lax.fori_loop(8, 12, drain_wide, 0)
        lax.fori_loop(8, 14, drain_shared, 0)
        add_residual()
        w_wait(13, 14)
        w_start(18)
        load(6, 0).start()
        load(6, 0).wait()
        add(6, 0, 0)
        w_wait(15, 18)
        load(7, 1).start()
        add(6, 1, 0)
        load(7, 1).wait()
        add(7, 0, 1)
        finish(0, 0, 4)
        add(7, 1, 1, subs=(0, 1))
        finish(1, 0, 2)
        add(7, 1, 1, subs=(2,))
        finish(1, 2, 1)
        tail = pl.ds(rows - piece, piece)
        part_ref[...] = acc[tail]
        last_copy(3).wait_recv()
        act_ref[...] = gin[6, tail]

    pl.run_scoped(
        consume,
        pltpu.VMEM((rows, width), F32),
        pltpu.SemaphoreType.DMA((2,)),
        pltpu.SemaphoreType.DMA,
    )

    for e in range(13, len(events)):
        w_copy(e).wait_send()
    lax.fori_loop(4, 7, drain_near, 0)
    for s in range(4):
        last_copy(s).wait_send()


def tail_kernel(h_ref, n_ref, w_ref, part_ref, act_ref, gain_ref, h_out, n_out, total, tail_h, tail_n, sem):
    rows, width = h_ref.shape
    piece = part_ref.shape[0]
    done, tail = pl.ds(0, rows - piece), pl.ds(rows - piece, piece)
    copies = [
        pltpu.make_async_copy(h_ref.at[done], h_out.at[done], sem.at[0]),
        pltpu.make_async_copy(n_ref.at[done], n_out.at[done], sem.at[1]),
        pltpu.make_async_copy(tail_h, h_out.at[tail], sem.at[2]),
        pltpu.make_async_copy(tail_n, n_out.at[tail], sem.at[3]),
    ]
    copies[0].start()
    copies[1].start()
    tile_n, sub = 512, 32

    @pl.loop(0, width // tile_n)
    def _(n):
        tile = pl.ds(pl.multiple_of(n * tile_n, tile_n), tile_n)
        prod = jnp.dot(act_ref[...], w_ref[:, tile], preferred_element_type=F32)
        total[:, tile] = part_ref[:, tile] + prod.astype(BF16).astype(F32)

    @pl.loop(0, piece // sub)
    def _(i):
        at = pl.ds(pl.multiple_of(i * sub, sub), sub)
        h32 = total[at]
        mean_sq = jnp.sum(h32 * h32, axis=-1, keepdims=True) * (1.0 / width)
        tail_h[at] = h32.astype(BF16)
        tail_n[at] = (h32 * lax.rsqrt(mean_sq + EPS) * gain_ref[...]).astype(BF16)

    copies[2].start()
    copies[3].start()
    for copy in copies:
        copy.wait()


def solution(mesh):
    def local_block(x_in, w_gate, w_up, w_down, residual, norm_gain):
        rows, width = residual.shape
        cols = w_gate.shape[1]
        any_spec = pl.BlockSpec(memory_space=pl.ANY)
        vm = pl.BlockSpec(memory_space=pltpu.VMEM)
        piece = rows // 8
        gain = norm_gain.reshape(1, width)
        *held, _ = pl.pallas_call(
            block_kernel,
            out_shape=(
                pltpu.VMEM((rows, width), BF16),
                pltpu.VMEM((rows, width), BF16),
                pltpu.VMEM((rows, width), BF16),
                pltpu.VMEM((piece, width), F32),
                pltpu.VMEM((piece, cols), BF16),
                jax.ShapeDtypeStruct((8, rows, width), BF16),
            ),
            in_specs=[any_spec] * 5 + [vm],
            out_specs=(vm,) * 5 + (any_spec,),
            scratch_shapes=[
                pltpu.VMEM((14, rows // 2, cols), BF16),
                pltpu.VMEM((7, rows, cols), BF16),
                pltpu.SemaphoreType.DMA((19,)),
                pltpu.SemaphoreType.DMA((19,)),
                pltpu.SemaphoreType.DMA((18,)),
                pltpu.SemaphoreType.DMA((20,)),
                pltpu.SemaphoreType.DMA((12,)),
                pltpu.SemaphoreType.DMA((12,)),
                pltpu.SemaphoreType.DMA((6,)),
                pltpu.SemaphoreType.DMA((12,)),
            ],
            compiler_params=pltpu.CompilerParams(collective_id=0, has_side_effects=True, vmem_limit_bytes=46_200_000),
        )(x_in, w_gate, w_up, w_down, residual, gain)
        return pl.pallas_call(
            tail_kernel,
            out_shape=(jax.ShapeDtypeStruct((rows, width), BF16), jax.ShapeDtypeStruct((rows, width), BF16)),
            in_specs=[vm] * 6,
            out_specs=(any_spec, any_spec),
            scratch_shapes=[
                pltpu.VMEM((piece, width), F32),
                pltpu.VMEM((piece, width), BF16),
                pltpu.VMEM((piece, width), BF16),
                pltpu.SemaphoreType.DMA((4,)),
            ],
            compiler_params=pltpu.CompilerParams(vmem_limit_bytes=8_000_000),
        )(*held, gain)

    row_spec = P(("data", "tp"), None)
    return jax.shard_map(local_block, mesh=mesh, in_specs=(P("data", None), P(None, "tp"), P(None, "tp"), P("tp", None), row_spec, P(None)), out_specs=(row_spec, row_spec), check_vma=False)
```

```python
import functools

import jax
import jax.numpy as jnp
from jax import lax
from jax.experimental import pallas as pl
from jax.experimental.pallas import tpu as pltpu
from jax.sharding import PartitionSpec as P

EPS = 1e-5
MESH = pl.DeviceIdType.MESH
F32 = jnp.float32
BF16 = jnp.bfloat16


def block_kernel(x_ref, wg_ref, wu_ref, wd_ref, res_ref, gain_ref, h_ref, n_ref, wbuf, part_ref, act_ref, wall_ref, gout, gin, w_send, w_recv, g_send, g_recv, q_send, q_recv, s_send, s_recv):
    p = lax.axis_index("tp")
    z = lax.axis_index("data")
    core, px, py = p % 2, (p // 2) % 2, p // 4
    rows = wd_ref.shape[0]
    half, quarter, piece = rows // 2, rows // 4, rows // 8
    cols = wg_ref.shape[1]
    width = wd_ref.shape[1]
    blocks = 16
    own_cols = cols * 3 // 4
    share = cols - own_cols
    depth = wg_ref.shape[0]
    deep = depth // 6

    def peer(r):
        return p + (r % 2) * (1 - 2 * core) + ((r // 2) % 2) * (2 - 4 * px) + (r // 4) * (4 - 8 * py)

    def tp(r):
        return {"tp": peer(r)}

    twin = {"data": 1 - z}

    mine, other = z * half, (1 - z) * half
    first = 13 * rows // 64
    q0, q1 = pl.ds(mine, first), pl.ds(mine + first, half - first)
    hm, ho = pl.ds(mine, half), pl.ds(other, half)
    whole = pl.ds(0, rows)
    events = [
        (0, 2, q0, tp(2)),
        (0, 2, q1, tp(2)),
        (0, 4, q1, tp(4)),
        (0, 4, q0, tp(4)),
        (0, 1, whole, tp(1)),
        (2, 6, q0, tp(4)),
        (2, 2, q0, twin),
        (4, 6, q1, tp(2)),
        (4, 4, q1, twin),
        (2, 2, q1, twin),
        (2, 3, hm, tp(1)),
        (4, 4, q0, twin),
        (4, 5, hm, tp(1)),
        (6, 6, q0, twin),
        (6, 6, q1, twin),
        (6, 7, hm, tp(1)),
        (2, 3, ho, tp(1)),
        (4, 5, ho, tp(1)),
        (6, 7, ho, tp(1)),
    ]

    def w_copy(e):
        src, dst, where, target = events[e]
        src_ref = wd_ref.at[where] if src == 0 else wall_ref.at[src, where]
        return pltpu.make_async_remote_copy(src_ref=src_ref, dst_ref=wall_ref.at[dst, where], send_sem=w_send.at[0], recv_sem=w_recv.at[e], device_id=target, device_id_type=MESH)

    def w_start(*ids):
        for e in ids:
            w_copy(e).start()

    def w_wait(*ids):
        for e in ids:
            w_copy(e).wait_recv()

    def place(j):
        g = j // 4
        return jnp.where(j < 12, 2 + 4 * g - 6 * (g // 2) + (j // 2) % 2, 1 - (j - 12) // 2), j % 2

    def g_copy(j, r, h, count):
        src = gout.at[j, :, pl.ds(0, count)]
        dst = gin.at[r - 1, pl.ds(h * half, half), pl.ds(0, count)]
        return pltpu.make_async_remote_copy(src_ref=src, dst_ref=dst, send_sem=g_send.at[jnp.where(j < 8, 0, jnp.where(j < 12, 1, j - 10))], recv_sem=g_recv.at[2 * r + h - 2], device_id=tp(r), device_id_type=MESH)

    def g_start(j, count):
        r, h = place(j)
        g_copy(j, r, h, count).start()

    def g_wait_send(j, count):
        r, h = place(j)
        g_copy(j, r, h, count).wait_send()

    def last_copy(s):
        where = pl.ds(s * piece, piece)
        src = gout.at[7, where, pl.ds(0, own_cols)]
        dst = gin.at[6, pl.ds(half + s * piece, piece), pl.ds(0, own_cols)]
        return pltpu.make_async_remote_copy(src_ref=src, dst_ref=dst, send_sem=g_send.at[0], recv_sem=g_recv.at[13 + s], device_id=tp(7), device_id_type=MESH)

    def stage(j):
        return jnp.where(j < 12, j - 4, j - 10)

    def s_copy(j, r, h):
        shared = pl.ds(own_cols, share)
        return pltpu.make_async_remote_copy(src_ref=gout.at[stage(j), :, shared], dst_ref=gin.at[r + 1, pl.ds(h * half, half), shared], send_sem=s_send.at[0], recv_sem=s_recv.at[2 * (r - r // 4 * 2) + h - 2], device_id=tp(r), device_id_type=MESH)

    def s_start(j):
        r, h = place(j)
        s_copy(j, r, h).start()

    def q_where(k):
        at = (k % 2) * (depth // 2) + (3 * z + k // 2) * share
        return wbuf.at[pl.ds(0, deep), pl.ds(pl.multiple_of(at, share), share)]

    def q_copy(k, src, sem, target):
        return pltpu.make_async_remote_copy(src_ref=src, dst_ref=q_where(k), send_sem=q_send.at[1 if target is twin else 0], recv_sem=q_recv.at[sem], device_id=target, device_id_type=MESH)

    def q_first(k):
        src = (wg_ref, wu_ref)[k % 2]
        at = pl.multiple_of((3 * z + k // 2) * deep, deep)
        return q_copy(k, src.at[pl.ds(at, deep), pl.ds(own_cols, share)], k, tp(2))

    def q_arrived(k):
        return q_copy(k, q_where(k), k, tp(2))

    def q_swap(k):
        return q_copy(k, q_where(k), 6, twin)

    def produce(wg, wu, x_sem, wg_sem, wu_sem):
        def x_copy(j):
            r, h = place(j)
            start = pl.multiple_of(peer(r) * rows + h * half, half)
            return pltpu.make_async_copy(x_ref.at[pl.ds(start, half)], n_ref.at[pl.ds((j % 2) * half, half)], x_sem.at[j % 2])

        wg_copy = pltpu.make_async_copy(wg_ref, wg, wg_sem)
        wu_copy = pltpu.make_async_copy(wu_ref, wu, wu_sem)
        x_copy(0).start()
        wg_copy.start()
        wu_copy.start()

        barrier = pltpu.get_barrier_semaphore()
        for r in range(1, 8):
            pl.semaphore_signal(barrier, inc=1, device_id=tp(r), device_id_type=MESH)
        pl.semaphore_signal(barrier, inc=1, device_id=twin, device_id_type=MESH)
        pl.semaphore_wait(barrier, 8)

        for k in range(6):
            q_first(k).start()
        w_start(0, 2, 1, 3, 4)
        wg_copy.wait()
        wu_copy.wait()

        def send_near(j, carry):
            g_start(j, own_cols)
            return carry

        def send_wide(j, carry):
            g_start(j, cols)
            s_start(j)
            return carry

        def step(j, carry):
            x_copy(j).wait()
            slot = jnp.where(j < 14, j, j - 2)
            r, h = place(j)
            xrows = pl.ds(pl.multiple_of((j % 2) * half, half), half)

            @pl.when(j + 1 < blocks)
            def _():
                x_copy(j + 1).start()

            @pl.when(j >= 14)
            def _():
                g_wait_send(j - 2, cols)

            @pl.loop(0, 3)
            def _(n):
                tile = pl.ds(pl.multiple_of(n * 256, 256), 256)
                xb = n_ref[xrows]
                gate = jnp.dot(xb, wg[:, tile], preferred_element_type=F32)
                up = jnp.dot(xb, wu[:, tile], preferred_element_type=F32)
                gout[slot, :, tile] = (jax.nn.silu(gate) * up).astype(BF16)

            @pl.when(j >= 8)
            def _():
                tile = pl.ds(own_cols, share)
                xb = n_ref[xrows]
                gate = jnp.dot(xb, wg[:, tile], preferred_element_type=F32)
                up = jnp.dot(xb, wu[:, tile], preferred_element_type=F32)
                gout[slot, :, tile] = (jax.nn.silu(gate) * up).astype(BF16)

            @pl.when(j < 6)
            def _():
                q_arrived(j).wait_recv()
                q_swap(j).start()

            @pl.when(j == 6)
            def _():
                w_wait(2)
                w_start(7, 8)

            @pl.when(j == 7)
            def _():
                lax.fori_loop(0, 7, send_near, 0)
                for s in range(4):
                    last_copy(s).start()

            @pl.when(j == 8)
            def _():
                mine_q = wbuf.at[pl.ds(0, deep), pl.ds(0, depth // 2)]
                pltpu.make_async_remote_copy(src_ref=mine_q, dst_ref=mine_q, send_sem=q_send.at[1], recv_sem=q_recv.at[6], device_id=twin, device_id_type=MESH).wait()

            @pl.when(j == 9)
            def _():
                w_wait(0)
                w_start(5, 6)

            @pl.when(j >= 8)
            def _():
                @pl.loop(0, 4)
                def _(t):
                    top = t * piece
                    xt = pl.ds(pl.multiple_of((j % 2) * half + top, piece), piece)

                    def product(base):
                        total = None
                        for k in range(6):
                            part = jnp.dot(n_ref[xt, k * deep:(k + 1) * deep], wbuf[0:deep, base + k * share:base + (k + 1) * share], preferred_element_type=F32)
                            total = part if total is None else total + part
                        return total

                    val = (jax.nn.silu(product(0)) * product(depth // 2)).astype(BF16)

                    @pl.when(j < 14)
                    def _():
                        gout[stage(j), pl.ds(pl.multiple_of(top, piece), piece), own_cols:] = val

                    @pl.when(j >= 14)
                    def _():
                        gin[1, pl.ds(pl.multiple_of(h * half + top, piece), piece), own_cols:] = val

            @pl.when(j == 9)
            def _():
                lax.fori_loop(8, 10, send_wide, 0)

            @pl.when((j >= 10) & (j < 14))
            def _():
                g_start(j, cols)
                s_start(j)

            @pl.when(j == 10)
            def _():
                w_wait(3)
                w_start(11, 12)

            @pl.when(j == 13)
            def _():
                w_wait(1)
                w_start(9, 10)

            return carry

        lax.fori_loop(0, blocks, step, 0)

    pl.run_scoped(
        produce,
        pltpu.VMEM(wg_ref.shape, BF16),
        pltpu.VMEM(wu_ref.shape, BF16),
        pltpu.SemaphoreType.DMA((2,)),
        pltpu.SemaphoreType.DMA,
        pltpu.SemaphoreType.DMA,
    )

    def consume(acc, wb_sem, res_sem):
        tile_n = 512

        def load(r, slot):
            src = wd_ref if r == 0 else wall_ref.at[r]
            return pltpu.make_async_copy(src, (h_ref, wbuf)[slot], wb_sem.at[slot])

        def add(r, h, slot, first=False, subs=(0, 1, 2, 3)):
            if r:
                if (r, h) == (7, 1):
                    for s in subs:
                        last_copy(s).wait_recv()
                else:
                    g_copy(0, r, h, own_cols if r in (2, 3, 6, 7) else cols).wait_recv()
            if r in (3, 6, 7) and subs[0] == 0:
                s_copy(8, r - 2, h).wait_recv()
            count = piece * len(subs)
            inner = pl.ds(subs[0] * piece, count)
            outer = pl.ds(h * half + subs[0] * piece, count)

            @pl.loop(0, width // tile_n)
            def _(n):
                tile = pl.ds(pl.multiple_of(n * tile_n, tile_n), tile_n)
                act = gout[12 + h, inner] if r == 0 else gin[r - 1, outer]
                prod = jnp.dot(act, (h_ref, wbuf)[slot][:, tile], preferred_element_type=F32).astype(BF16).astype(F32)
                if first:
                    acc[outer, tile] = prod
                else:
                    acc[outer, tile] += prod

        def add_residual():
            copy = pltpu.make_async_copy(res_ref, h_ref, res_sem)
            copy.start()
            copy.wait()

            @pl.loop(0, rows // 32)
            def _(i):
                at = pl.ds(pl.multiple_of(i * 32, 32), 32)
                acc[at] += h_ref[at].astype(F32)

        sub = 32

        def finish(h, s0, count):
            @pl.loop(0, count * piece // sub)
            def _(i):
                there = pl.ds(pl.multiple_of(h * half + s0 * piece + i * sub, sub), sub)
                h32 = acc[there]
                mean_sq = jnp.sum(h32 * h32, axis=-1, keepdims=True) * (1.0 / width)
                h_ref[there] = h32.astype(BF16)
                n_ref[there] = (h32 * lax.rsqrt(mean_sq + EPS) * gain_ref[...]).astype(BF16)

        def run(steps, first=False):
            load(steps[0][0], 0).start()
            for i, (r, halves) in enumerate(steps):
                load(r, i % 2).wait()
                if i + 1 < len(steps):
                    load(steps[i + 1][0], (i + 1) % 2).start()
                for h in halves:
                    add(r, h, i % 2, first and i == 0)

        w_wait(5)
        w_start(13)
        w_wait(4)
        run([(0, (0, 1)), (1, (0, 1))], first=True)
        w_wait(7)
        w_start(14, 15)
        w_wait(8, 11)
        w_start(17)
        run([(4, (0, 1))])
        w_wait(12, 17)
        run([(5, (0, 1))])
        w_wait(6, 9)
        w_start(16)
        run([(2, (0, 1))])
        w_wait(10, 16)
        run([(3, (0, 1))])
        add_residual()
        early = pltpu.make_async_copy(wall_ref.at[6, hm], h_ref.at[hm], res_sem)
        late = pltpu.make_async_copy(wall_ref.at[6, ho], h_ref.at[ho], wb_sem.at[0])
        early.start()
        w_wait(13, 14)
        w_start(18)
        late.start()
        early.wait()
        late.wait()
        add(6, 0, 0)
        w_wait(15, 18)
        load(7, 1).start()
        add(6, 1, 0)
        load(7, 1).wait()
        add(7, 0, 1)
        finish(0, 0, 4)
        add(7, 1, 1, subs=(0, 1))
        finish(1, 0, 2)
        add(7, 1, 1, subs=(2,))
        finish(1, 2, 1)
        tail = pl.ds(rows - piece, piece)
        part_ref[...] = acc[tail]
        last_copy(3).wait_recv()
        act_ref[...] = gin[6, tail]

    pl.run_scoped(
        consume,
        pltpu.VMEM((rows, width), F32),
        pltpu.SemaphoreType.DMA((2,)),
        pltpu.SemaphoreType.DMA,
    )

    def sent(ref, sem):
        pltpu.make_async_remote_copy(src_ref=ref, dst_ref=ref, send_sem=sem, recv_sem=w_recv.at[0], device_id=tp(1), device_id_type=MESH).wait_send()

    sent(wall_ref.at[pl.ds(0, 7)], w_send.at[0])
    sent(wbuf.at[pl.ds(0, deep), pl.ds(0, depth // 2)], q_send.at[0])
    sent(gout.at[pl.ds(0, 8), :, pl.ds(0, own_cols)], g_send.at[0])
    sent(gout.at[pl.ds(8, 4)], g_send.at[1])
    sent(gout.at[pl.ds(0, 6), :, pl.ds(own_cols, share)], s_send.at[0])


def tail_kernel(h_ref, n_ref, w_ref, part_ref, act_ref, gain_ref, h_out, n_out, total, tail_h, tail_n, sem):
    rows, width = h_ref.shape
    piece = part_ref.shape[0]
    done, tail = pl.ds(0, rows - piece), pl.ds(rows - piece, piece)
    copies = [
        pltpu.make_async_copy(h_ref.at[done], h_out.at[done], sem.at[0]),
        pltpu.make_async_copy(n_ref.at[done], n_out.at[done], sem.at[1]),
        pltpu.make_async_copy(tail_h, h_out.at[tail], sem.at[2]),
        pltpu.make_async_copy(tail_n, n_out.at[tail], sem.at[3]),
    ]
    copies[0].start()
    copies[1].start()
    tile_n, sub = 512, 32

    @pl.loop(0, width // tile_n)
    def _(n):
        tile = pl.ds(pl.multiple_of(n * tile_n, tile_n), tile_n)
        prod = jnp.dot(act_ref[...], w_ref[:, tile], preferred_element_type=F32)
        total[:, tile] = part_ref[:, tile] + prod.astype(BF16).astype(F32)

    @pl.loop(0, piece // sub)
    def _(i):
        at = pl.ds(pl.multiple_of(i * sub, sub), sub)
        h32 = total[at]
        mean_sq = jnp.sum(h32 * h32, axis=-1, keepdims=True) * (1.0 / width)
        tail_h[at] = h32.astype(BF16)
        tail_n[at] = (h32 * lax.rsqrt(mean_sq + EPS) * gain_ref[...]).astype(BF16)

    copies[2].start()
    copies[3].start()
    for copy in copies:
        copy.wait()


def solution(mesh):
    def local_block(x_in, w_gate, w_up, w_down, residual, norm_gain):
        rows, width = residual.shape
        cols = w_gate.shape[1]
        any_spec = pl.BlockSpec(memory_space=pl.ANY)
        vm = pl.BlockSpec(memory_space=pltpu.VMEM)
        piece = rows // 8
        gain = norm_gain.reshape(1, width)
        *held, _ = pl.pallas_call(
            block_kernel,
            out_shape=(
                pltpu.VMEM((rows, width), BF16),
                pltpu.VMEM((rows, width), BF16),
                pltpu.VMEM((rows, width), BF16),
                pltpu.VMEM((piece, width), F32),
                pltpu.VMEM((piece, cols), BF16),
                jax.ShapeDtypeStruct((8, rows, width), BF16),
            ),
            in_specs=[any_spec] * 5 + [vm],
            out_specs=(vm,) * 5 + (any_spec,),
            scratch_shapes=[
                pltpu.VMEM((14, rows // 2, cols), BF16),
                pltpu.VMEM((7, rows, cols), BF16),
                pltpu.SemaphoreType.DMA((1,)),
                pltpu.SemaphoreType.DMA((19,)),
                pltpu.SemaphoreType.DMA((4,)),
                pltpu.SemaphoreType.DMA((17,)),
                pltpu.SemaphoreType.DMA((2,)),
                pltpu.SemaphoreType.DMA((7,)),
                pltpu.SemaphoreType.DMA((1,)),
                pltpu.SemaphoreType.DMA((6,)),
            ],
            compiler_params=pltpu.CompilerParams(collective_id=0, has_side_effects=True, vmem_limit_bytes=46_200_000),
        )(x_in, w_gate, w_up, w_down, residual, gain)
        return pl.pallas_call(
            tail_kernel,
            out_shape=(jax.ShapeDtypeStruct((rows, width), BF16), jax.ShapeDtypeStruct((rows, width), BF16)),
            in_specs=[vm] * 6,
            out_specs=(any_spec, any_spec),
            scratch_shapes=[
                pltpu.VMEM((piece, width), F32),
                pltpu.VMEM((piece, width), BF16),
                pltpu.VMEM((piece, width), BF16),
                pltpu.SemaphoreType.DMA((4,)),
            ],
            compiler_params=pltpu.CompilerParams(vmem_limit_bytes=8_000_000),
        )(*held, gain)

    row_spec = P(("data", "tp"), None)
    return jax.shard_map(local_block, mesh=mesh, in_specs=(P("data", None), P(None, "tp"), P(None, "tp"), P("tp", None), row_spec, P(None)), out_specs=(row_spec, row_spec), check_vma=False)
```

```python
import functools

import jax
import jax.numpy as jnp
from jax import lax
from jax.experimental import pallas as pl
from jax.experimental.pallas import tpu as pltpu
from jax.sharding import PartitionSpec as P

EPS = 1e-5
MESH = pl.DeviceIdType.MESH
F32 = jnp.float32
BF16 = jnp.bfloat16


def block_kernel(x_ref, wg_ref, wu_ref, wd_ref, res_ref, gain_ref, h_ref, n_ref, wbuf, part_ref, act_ref, wall_ref, gout, gin, w_send, w_recv, g_send, g_recv, q_send, q_recv, s_send, s_recv):
    p = lax.axis_index("tp")
    z = lax.axis_index("data")
    core, px, py = p % 2, (p // 2) % 2, p // 4
    rows = wd_ref.shape[0]
    half, quarter, piece = rows // 2, rows // 4, rows // 8
    cols = wg_ref.shape[1]
    width = wd_ref.shape[1]
    blocks = 16
    own_cols = cols * 3 // 4
    share = cols - own_cols
    depth = wg_ref.shape[0]
    deep = depth // 6

    def peer(r):
        return p + (r % 2) * (1 - 2 * core) + ((r // 2) % 2) * (2 - 4 * px) + (r // 4) * (4 - 8 * py)

    def tp(r):
        return {"tp": peer(r)}

    twin = {"data": 1 - z}

    mine, other = z * half, (1 - z) * half
    first = 13 * rows // 64
    q0, q1 = pl.ds(mine, first), pl.ds(mine + first, half - first)
    hm, ho = pl.ds(mine, half), pl.ds(other, half)
    whole = pl.ds(0, rows)
    events = [
        (0, 2, q0, tp(2)),
        (0, 2, q1, tp(2)),
        (0, 4, q1, tp(4)),
        (0, 4, q0, tp(4)),
        (0, 1, whole, tp(1)),
        (2, 6, q0, tp(4)),
        (2, 2, q0, twin),
        (4, 6, q1, tp(2)),
        (4, 4, q1, twin),
        (2, 2, q1, twin),
        (2, 3, hm, tp(1)),
        (4, 4, q0, twin),
        (4, 5, hm, tp(1)),
        (6, 6, q0, twin),
        (6, 6, q1, twin),
        (6, 7, hm, tp(1)),
        (2, 3, ho, tp(1)),
        (4, 5, ho, tp(1)),
        (6, 7, ho, tp(1)),
    ]

    def w_copy(e):
        src, dst, where, target = events[e]
        src_ref = wd_ref.at[where] if src == 0 else wall_ref.at[src, where]
        return pltpu.make_async_remote_copy(src_ref=src_ref, dst_ref=wall_ref.at[dst, where], send_sem=w_send.at[0], recv_sem=w_recv.at[{9: 6, 11: 8, 14: 9, 13: 9, 16: 10, 17: 12, 18: 11, 15: 11}.get(e, e)], device_id=target, device_id_type=MESH)

    def w_both(e, count):
        pair = wall_ref.at[1, pl.ds(0, count)]
        sem = {13: 9, 15: 11}.get(e, e)
        pltpu.make_async_remote_copy(src_ref=pair, dst_ref=pair, send_sem=w_send.at[0], recv_sem=w_recv.at[sem], device_id=twin, device_id_type=MESH).wait_recv()

    def w_start(*ids):
        for e in ids:
            w_copy(e).start()

    def w_wait(*ids):
        for e in ids:
            w_copy(e).wait_recv()

    def place(j):
        g = j // 4
        return jnp.where(j < 12, 2 + 4 * g - 6 * (g // 2) + (j // 2) % 2, 1 - (j - 12) // 2), j % 2

    def g_copy(j, r, h, count):
        src = gout.at[j, :, pl.ds(0, count)]
        dst = gin.at[r - 1, pl.ds(h * half, half), pl.ds(0, count)]
        return pltpu.make_async_remote_copy(src_ref=src, dst_ref=dst, send_sem=g_send.at[jnp.where(j < 8, 0, jnp.where(j < 12, 1, j - 10))], recv_sem=g_recv.at[2 * r + h - 2], device_id=tp(r), device_id_type=MESH)

    def g_start(j, count):
        r, h = place(j)
        g_copy(j, r, h, count).start()

    def g_wait_send(j, count):
        r, h = place(j)
        g_copy(j, r, h, count).wait_send()

    def last_copy(s):
        where = pl.ds(s * piece, piece)
        src = gout.at[7, where, pl.ds(0, own_cols)]
        dst = gin.at[6, pl.ds(half + s * piece, piece), pl.ds(0, own_cols)]
        return pltpu.make_async_remote_copy(src_ref=src, dst_ref=dst, send_sem=g_send.at[0], recv_sem=g_recv.at[13 + s], device_id=tp(7), device_id_type=MESH)

    def stage(j):
        return jnp.where(j < 12, j - 4, j - 10)

    def s_copy(j, r, h):
        shared = pl.ds(own_cols, share)
        return pltpu.make_async_remote_copy(src_ref=gout.at[stage(j), :, shared], dst_ref=gin.at[r + 1, pl.ds(h * half, half), shared], send_sem=s_send.at[0], recv_sem=s_recv.at[r - r // 4 * 2 - 1], device_id=tp(r), device_id_type=MESH)

    def s_start(j):
        r, h = place(j)
        s_copy(j, r, h).start()

    def q_where(k):
        at = (k % 2) * (depth // 2) + (3 * z + k // 2) * share
        return wbuf.at[pl.ds(0, deep), pl.ds(pl.multiple_of(at, share), share)]

    def q_copy(k, src, sem, target):
        return pltpu.make_async_remote_copy(src_ref=src, dst_ref=q_where(k), send_sem=q_send.at[1 if target is twin else 0], recv_sem=q_recv.at[sem], device_id=target, device_id_type=MESH)

    def q_first(k):
        src = (wg_ref, wu_ref)[k % 2]
        at = pl.multiple_of((3 * z + k // 2) * deep, deep)
        return q_copy(k, src.at[pl.ds(at, deep), pl.ds(own_cols, share)], k, tp(2))

    def q_arrived(k):
        return q_copy(k, q_where(k), k, tp(2))

    def q_swap(k):
        return q_copy(k, q_where(k), 6, twin)

    def produce(wg, wu, x_sem, wg_sem, wu_sem):
        def x_copy(j):
            r, h = place(j)
            start = pl.multiple_of(peer(r) * rows + h * half, half)
            return pltpu.make_async_copy(x_ref.at[pl.ds(start, half)], n_ref.at[pl.ds((j % 2) * half, half)], x_sem.at[j % 2])

        wg_copy = pltpu.make_async_copy(wg_ref, wg, wg_sem)
        wu_copy = pltpu.make_async_copy(wu_ref, wu, wu_sem)
        x_copy(0).start()
        wg_copy.start()
        wu_copy.start()

        barrier = pltpu.get_barrier_semaphore()
        for r in range(1, 8):
            pl.semaphore_signal(barrier, inc=1, device_id=tp(r), device_id_type=MESH)
        pl.semaphore_signal(barrier, inc=1, device_id=twin, device_id_type=MESH)
        pl.semaphore_wait(barrier, 8)

        for k in range(6):
            q_first(k).start()
        w_start(0, 2, 1, 3, 4)
        wg_copy.wait()
        wu_copy.wait()

        def send_near(j, carry):
            g_start(j, own_cols)
            return carry

        def send_wide(j, carry):
            g_start(j, cols)
            s_start(j)
            return carry

        def step(j, carry):
            x_copy(j).wait()
            slot = jnp.where(j < 14, j, j - 2)
            r, h = place(j)
            xrows = pl.ds(pl.multiple_of((j % 2) * half, half), half)

            @pl.when(j + 1 < blocks)
            def _():
                x_copy(j + 1).start()

            @pl.when(j >= 14)
            def _():
                g_wait_send(j - 2, cols)

            @pl.loop(0, 3)
            def _(n):
                tile = pl.ds(pl.multiple_of(n * 256, 256), 256)
                xb = n_ref[xrows]
                gate = jnp.dot(xb, wg[:, tile], preferred_element_type=F32)
                up = jnp.dot(xb, wu[:, tile], preferred_element_type=F32)
                gout[slot, :, tile] = (jax.nn.silu(gate) * up).astype(BF16)

            @pl.when(j >= 8)
            def _():
                tile = pl.ds(own_cols, share)
                xb = n_ref[xrows]
                gate = jnp.dot(xb, wg[:, tile], preferred_element_type=F32)
                up = jnp.dot(xb, wu[:, tile], preferred_element_type=F32)
                gout[slot, :, tile] = (jax.nn.silu(gate) * up).astype(BF16)

            @pl.when(j < 6)
            def _():
                q_arrived(j).wait_recv()
                q_swap(j).start()

            @pl.when(j == 6)
            def _():
                w_wait(2)
                w_start(7, 8)

            @pl.when(j == 7)
            def _():
                lax.fori_loop(0, 7, send_near, 0)
                for s in range(4):
                    last_copy(s).start()

            @pl.when(j == 8)
            def _():
                mine_q = wbuf.at[pl.ds(0, deep), pl.ds(0, depth // 2)]
                pltpu.make_async_remote_copy(src_ref=mine_q, dst_ref=mine_q, send_sem=q_send.at[1], recv_sem=q_recv.at[6], device_id=twin, device_id_type=MESH).wait()

            @pl.when(j == 9)
            def _():
                w_wait(0)
                w_start(5, 6)

            @pl.when(j >= 8)
            def _():
                @pl.loop(0, 4)
                def _(t):
                    top = t * piece
                    xt = pl.ds(pl.multiple_of((j % 2) * half + top, piece), piece)

                    def product(base):
                        total = None
                        for k in range(6):
                            part = jnp.dot(n_ref[xt, k * deep:(k + 1) * deep], wbuf[0:deep, base + k * share:base + (k + 1) * share], preferred_element_type=F32)
                            total = part if total is None else total + part
                        return total

                    val = (jax.nn.silu(product(0)) * product(depth // 2)).astype(BF16)

                    @pl.when(j < 14)
                    def _():
                        gout[stage(j), pl.ds(pl.multiple_of(top, piece), piece), own_cols:] = val

                    @pl.when(j >= 14)
                    def _():
                        gin[1, pl.ds(pl.multiple_of(h * half + top, piece), piece), own_cols:] = val

            @pl.when(j == 9)
            def _():
                lax.fori_loop(8, 10, send_wide, 0)

            @pl.when((j >= 10) & (j < 14))
            def _():
                g_start(j, cols)
                s_start(j)

            @pl.when(j == 10)
            def _():
                w_wait(3)
                w_start(11, 12)

            @pl.when(j == 13)
            def _():
                w_wait(1)
                w_start(9, 10)

            return carry

        lax.fori_loop(0, blocks, step, 0)

    pl.run_scoped(
        produce,
        pltpu.VMEM(wg_ref.shape, BF16),
        pltpu.VMEM(wu_ref.shape, BF16),
        pltpu.SemaphoreType.DMA((2,)),
        pltpu.SemaphoreType.DMA,
        pltpu.SemaphoreType.DMA,
    )

    def consume(acc, wb_sem, res_sem):
        tile_n = 512

        def load(r, slot):
            src = wd_ref if r == 0 else wall_ref.at[r]
            return pltpu.make_async_copy(src, (h_ref, wbuf)[slot], wb_sem.at[slot])

        def add(r, h, slot, first=False, subs=(0, 1, 2, 3)):
            if r:
                if (r, h) == (7, 1):
                    for s in subs:
                        last_copy(s).wait_recv()
                else:
                    g_copy(0, r, h, own_cols if r in (2, 3, 6, 7) else cols).wait_recv()
            if r in (3, 6, 7) and h == 0:
                both = gin.at[r - 1, :, pl.ds(own_cols, share)]
                pltpu.make_async_remote_copy(src_ref=both, dst_ref=both, send_sem=s_send.at[0], recv_sem=s_recv.at[(3, 6, 7).index(r)], device_id=tp(r), device_id_type=MESH).wait_recv()
            count = piece * len(subs)
            inner = pl.ds(subs[0] * piece, count)
            outer = pl.ds(h * half + subs[0] * piece, count)

            @pl.loop(0, width // tile_n)
            def _(n):
                tile = pl.ds(pl.multiple_of(n * tile_n, tile_n), tile_n)
                act = gout[12 + h, inner] if r == 0 else gin[r - 1, outer]
                prod = jnp.dot(act, (h_ref, wbuf)[slot][:, tile], preferred_element_type=F32).astype(BF16).astype(F32)
                if first:
                    acc[outer, tile] = prod
                else:
                    acc[outer, tile] += prod

        def add_residual():
            copy = pltpu.make_async_copy(res_ref, h_ref, res_sem)
            copy.start()
            copy.wait()

            @pl.loop(0, rows // 32)
            def _(i):
                at = pl.ds(pl.multiple_of(i * 32, 32), 32)
                acc[at] += h_ref[at].astype(F32)

        sub = 32

        def finish(h, s0, count):
            @pl.loop(0, count * piece // sub)
            def _(i):
                there = pl.ds(pl.multiple_of(h * half + s0 * piece + i * sub, sub), sub)
                h32 = acc[there]
                mean_sq = jnp.sum(h32 * h32, axis=-1, keepdims=True) * (1.0 / width)
                h_ref[there] = h32.astype(BF16)
                n_ref[there] = (h32 * lax.rsqrt(mean_sq + EPS) * gain_ref[...]).astype(BF16)

        def run(steps, first=False):
            load(steps[0][0], 0).start()
            for i, (r, halves) in enumerate(steps):
                load(r, i % 2).wait()
                if i + 1 < len(steps):
                    load(steps[i + 1][0], (i + 1) % 2).start()
                for h in halves:
                    add(r, h, i % 2, first and i == 0)

        w_wait(5)
        w_start(13)
        w_wait(4)
        run([(0, (0, 1)), (1, (0, 1))], first=True)
        w_wait(7)
        w_start(14, 15)
        w_both(8, half)
        w_start(17)
        run([(4, (0, 1))])
        w_both(12, rows)
        run([(5, (0, 1))])
        w_both(6, half)
        w_start(16)
        run([(2, (0, 1))])
        w_both(10, rows)
        run([(3, (0, 1))])
        add_residual()
        early = pltpu.make_async_copy(wall_ref.at[6, hm], h_ref.at[hm], res_sem)
        late = pltpu.make_async_copy(wall_ref.at[6, ho], h_ref.at[ho], wb_sem.at[0])
        early.start()
        w_both(13, half)
        w_start(18)
        late.start()
        early.wait()
        late.wait()
        add(6, 0, 0)
        w_both(15, rows)
        load(7, 1).start()
        add(6, 1, 0)
        load(7, 1).wait()
        add(7, 0, 1)
        finish(0, 0, 4)
        add(7, 1, 1, subs=(0, 1))
        finish(1, 0, 2)
        add(7, 1, 1, subs=(2,))
        finish(1, 2, 1)
        tail = pl.ds(rows - piece, piece)
        part_ref[...] = acc[tail]
        last_copy(3).wait_recv()
        act_ref[...] = gin[6, tail]

    pl.run_scoped(
        consume,
        pltpu.VMEM((rows, width), F32),
        pltpu.SemaphoreType.DMA((2,)),
        pltpu.SemaphoreType.DMA,
    )

    def sent(ref, sem):
        pltpu.make_async_remote_copy(src_ref=ref, dst_ref=ref, send_sem=sem, recv_sem=w_recv.at[0], device_id=tp(1), device_id_type=MESH).wait_send()

    sent(wall_ref.at[pl.ds(0, 7)], w_send.at[0])
    sent(wbuf.at[pl.ds(0, deep), pl.ds(0, depth // 2)], q_send.at[0])
    sent(gout.at[pl.ds(0, 8), :, pl.ds(0, own_cols)], g_send.at[0])
    sent(gout.at[pl.ds(8, 4)], g_send.at[1])
    sent(gout.at[pl.ds(0, 6), :, pl.ds(own_cols, share)], s_send.at[0])


def tail_kernel(h_ref, n_ref, w_ref, part_ref, act_ref, gain_ref, h_out, n_out, total, tail_h, tail_n, sem):
    rows, width = h_ref.shape
    piece = part_ref.shape[0]
    done, tail = pl.ds(0, rows - piece), pl.ds(rows - piece, piece)
    copies = [
        pltpu.make_async_copy(h_ref.at[done], h_out.at[done], sem.at[0]),
        pltpu.make_async_copy(n_ref.at[done], n_out.at[done], sem.at[1]),
        pltpu.make_async_copy(tail_h, h_out.at[tail], sem.at[2]),
        pltpu.make_async_copy(tail_n, n_out.at[tail], sem.at[3]),
    ]
    copies[0].start()
    copies[1].start()
    tile_n, sub = 512, 32

    @pl.loop(0, width // tile_n)
    def _(n):
        tile = pl.ds(pl.multiple_of(n * tile_n, tile_n), tile_n)
        prod = jnp.dot(act_ref[...], w_ref[:, tile], preferred_element_type=F32)
        total[:, tile] = part_ref[:, tile] + prod.astype(BF16).astype(F32)

    @pl.loop(0, piece // sub)
    def _(i):
        at = pl.ds(pl.multiple_of(i * sub, sub), sub)
        h32 = total[at]
        mean_sq = jnp.sum(h32 * h32, axis=-1, keepdims=True) * (1.0 / width)
        tail_h[at] = h32.astype(BF16)
        tail_n[at] = (h32 * lax.rsqrt(mean_sq + EPS) * gain_ref[...]).astype(BF16)

    copies[2].start()
    copies[3].start()
    for copy in copies:
        copy.wait()


def solution(mesh):
    def local_block(x_in, w_gate, w_up, w_down, residual, norm_gain):
        rows, width = residual.shape
        cols = w_gate.shape[1]
        any_spec = pl.BlockSpec(memory_space=pl.ANY)
        vm = pl.BlockSpec(memory_space=pltpu.VMEM)
        piece = rows // 8
        gain = norm_gain.reshape(1, width)
        *held, _ = pl.pallas_call(
            block_kernel,
            out_shape=(
                pltpu.VMEM((rows, width), BF16),
                pltpu.VMEM((rows, width), BF16),
                pltpu.VMEM((rows, width), BF16),
                pltpu.VMEM((piece, width), F32),
                pltpu.VMEM((piece, cols), BF16),
                jax.ShapeDtypeStruct((8, rows, width), BF16),
            ),
            in_specs=[any_spec] * 5 + [vm],
            out_specs=(vm,) * 5 + (any_spec,),
            scratch_shapes=[
                pltpu.VMEM((14, rows // 2, cols), BF16),
                pltpu.VMEM((7, rows, cols), BF16),
                pltpu.SemaphoreType.DMA((1,)),
                pltpu.SemaphoreType.DMA((13,)),
                pltpu.SemaphoreType.DMA((4,)),
                pltpu.SemaphoreType.DMA((17,)),
                pltpu.SemaphoreType.DMA((2,)),
                pltpu.SemaphoreType.DMA((7,)),
                pltpu.SemaphoreType.DMA((1,)),
                pltpu.SemaphoreType.DMA((3,)),
            ],
            compiler_params=pltpu.CompilerParams(collective_id=0, has_side_effects=True, vmem_limit_bytes=46_200_000),
        )(x_in, w_gate, w_up, w_down, residual, gain)
        return pl.pallas_call(
            tail_kernel,
            out_shape=(jax.ShapeDtypeStruct((rows, width), BF16), jax.ShapeDtypeStruct((rows, width), BF16)),
            in_specs=[vm] * 6,
            out_specs=(any_spec, any_spec),
            scratch_shapes=[
                pltpu.VMEM((piece, width), F32),
                pltpu.VMEM((piece, width), BF16),
                pltpu.VMEM((piece, width), BF16),
                pltpu.SemaphoreType.DMA((4,)),
            ],
            compiler_params=pltpu.CompilerParams(vmem_limit_bytes=8_000_000),
        )(*held, gain)

    row_spec = P(("data", "tp"), None)
    return jax.shard_map(local_block, mesh=mesh, in_specs=(P("data", None), P(None, "tp"), P(None, "tp"), P("tp", None), row_spec, P(None)), out_specs=(row_spec, row_spec), check_vma=False)
```
